512 devices in a mesh: parts: 2 (over y), mem: 16 (over z), space: 16 (over x, core).
Axes of the slice: x: 8, y: 2, z: 16, core: 2. Of those that a mesh axis runs over, the one named last changes fastest.
The devices are a block of a 8x8x16 slice.
Arguments:
- ensemble: bfloat16 [64, 70, 32768], P('mem', None, ('parts', 'space')), parts along dimension 2, may hold values from -6 to 6
- transform: bfloat16 [128, 64], P('parts'), parts along dimension 0, may hold values from -0.75 to 0.75
- obs_operator: bfloat16 [16, 70], replicated, may hold values from -0.75 to 0.75
- obs_weight: float32 [16, 32768], P(None, ('parts', 'space')), parts along dimension 1, may hold values from 0.25 to 40, as said below
Outputs:
- analysis: bfloat16 [64, 70, 32768], P('mem', None, ('parts', 'space')), parts along dimension 2
- prior_gram: float32 [128, 64], P('parts'), parts along dimension 0
- posterior_gram: float32 [128, 64], P('parts'), parts along dimension 0
The draws below stay inside these ranges and needn't reach their ends.
There are 2 independent parts, one for each index of `parts`. The reference program is written for one: setup_inputs(seed, part) draws one part's arguments, and reference() takes and returns one part's arrays. A program takes and returns all parts, laid end to end along the dimension named above; an argument that names none is the same for every part. Nothing has to cross between parts.
Inputs may be any that keep to these rules, and one draw needn't show every extreme that they name: `obs_weight`: positive.
All inputs are finite; a program needn't handle non-finite values.
Results may differ from the reference program's by a relative error of at most 0.001.
Values may be sent and summed in bfloat16 or wider, within the bound.
No kernel may reach another device: no remote copies, remote signals or barrier semaphores. Data moves between devices by JAX's collectives and lax.ppermute only.
A program may use at most 64 MiB of HBM per device.

```python
import math
import jax
import jax.numpy as jnp
from jax import lax

MEMBERS = 64
VARS = 70
OBS = 16
CELLS = 16384


def draw_obs_weight(key, part):
    first_key = jax.random.fold_in(jax.random.fold_in(key, 11), 0)
    levels = jax.random.uniform(first_key, (OBS, CELLS), jnp.float32)
    position = jnp.arange(CELLS, dtype=jnp.float32) / max(CELLS - 1, 1)
    ramp = 1.0 + 2.0 * position
    return 0.5 * jnp.exp(levels * math.log(10.0)) * ramp[None, :]


def level_of(rng, shape, cuts, low, top_value):
    level = 1.0
    for dim, shards_of in cuts:
        steps = jax.random.uniform(jax.random.fold_in(jax.random.fold_in(rng, 6), dim), (shards_of,), jnp.float32, low / len(cuts), top_value / len(cuts))
        level = level * jnp.repeat(jnp.exp(steps), shape[dim] // shards_of).reshape((-1,) + (1,) * (len(shape) - 1 - dim))
    return level


def bell_draw(rng, shape, deviation, reach, shards=(), held_as=jnp.bfloat16):
    array = deviation * jax.random.normal(rng, shape, jnp.float32)
    if shards:
        array = array * level_of(rng, shape, shards, -0.22, 0.18)
    return jnp.clip(array, -reach, reach).astype(held_as)


def setup_inputs(seed: int = 0, part: int = 0) -> dict:
    seeds = jax.random.split(jax.random.key(seed), 5)
    part_splits = jax.random.split(jax.random.fold_in(seeds[4], part), 5)
    ensemble = bell_draw(part_splits[0], (MEMBERS, VARS, CELLS), 1.0, 6.0, ((0, 16), (2, 16)))
    transform = bell_draw(part_splits[1], (MEMBERS, MEMBERS), MEMBERS ** -0.5, 0.75)
    obs_operator = bell_draw(seeds[2], (OBS, VARS), VARS ** -0.5, 0.75)
    obs_weight = draw_obs_weight(jax.random.fold_in(jax.random.fold_in(seeds[4], part), 71), part)
    return dict(ensemble=ensemble, transform=transform, obs_operator=obs_operator, obs_weight=obs_weight)


def reference(ensemble, transform, obs_operator, obs_weight):
    mixing = transform.astype(jnp.float32)
    members = ensemble.astype(jnp.float32)
    member_mean = jnp.sum(members, axis=0) / MEMBERS
    combined = jnp.einsum("ij,ivc->jvc", mixing, members)
    keep_mean = 1.0 - jnp.sum(mixing, axis=0)
    analysis = (combined + member_mean[None, :, :] * keep_mean[:, None, None]).astype(jnp.bfloat16)
    observed = jnp.einsum("ov,mvc->moc", obs_operator.astype(jnp.float32), members)
    departures = observed - jnp.sum(observed, axis=0) / MEMBERS
    weighted = departures * obs_weight[None, :, :]
    gram_sum = jnp.einsum("ioc,joc->ij", weighted, departures, precision=lax.Precision.HIGHEST)
    prior_gram = gram_sum / jnp.sum(obs_weight)
    carried = jnp.dot(mixing.T, prior_gram, precision=lax.Precision.HIGHEST)
    posterior_gram = jnp.dot(carried, mixing, precision=lax.Precision.HIGHEST)
    return analysis, prior_gram, posterior_gram
```

```python
import jax
import jax.numpy as jnp
from jax import lax
from jax.sharding import PartitionSpec as P

MEMBERS = 64
LANES = 128
HIGHEST = lax.Precision.HIGHEST


def exchange(array, axis):
    return lax.all_to_all(array, axis, split_axis=0, concat_axis=0, tiled=True)


def to_all(array, axis, size):
    return exchange(jnp.broadcast_to(array[None], (size, *array.shape)), axis)


def per_device(mem, space, ensemble, transform, obs_operator, obs_weight):
    local, variables, cells = ensemble.shape
    quantities = obs_operator.shape[0]
    mixing = transform.astype(jnp.float32)
    tiles = cells // LANES
    halves = mem // tiles
    depth = variables // halves

    observed = jnp.einsum("ov,mvc->omc", obs_operator, ensemble, preferred_element_type=jnp.float32)
    by_quantity = exchange(observed.astype(jnp.bfloat16), "mem")

    blocks = ensemble.reshape(local, halves, depth, tiles, LANES)
    blocks = blocks.transpose(1, 3, 2, 0, 4).reshape(mem, depth, local, LANES)
    members = exchange(blocks, "mem")

    own = by_quantity.reshape(MEMBERS, cells).astype(jnp.float32)
    own_weights = lax.dynamic_slice_in_dim(obs_weight, lax.axis_index("mem"), 1, 0)
    departures = own - jnp.sum(own, axis=0, keepdims=True) / MEMBERS
    partial = lax.dot_general(
        departures * own_weights, departures, (((1,), (1,)), ((), ())), precision=HIGHEST
    )
    weight_sum = jnp.sum(own_weights)
    packed = jnp.concatenate([partial, jnp.broadcast_to(weight_sum, partial.shape)], axis=1)
    rows = MEMBERS // space
    packed = jnp.sum(exchange(packed.reshape(space, rows, LANES), "space"), axis=0)
    packed = jnp.sum(to_all(packed, "mem", mem), axis=0)
    packed = to_all(packed, "space", space).reshape(MEMBERS, LANES)
    prior_gram = packed[:, :MEMBERS] / packed[:, MEMBERS:]
    carried = jnp.dot(mixing.T, prior_gram, precision=HIGHEST)
    posterior_gram = jnp.dot(carried, mixing, precision=HIGHEST)

    members = members.transpose(1, 0, 2, 3).reshape(depth, MEMBERS, LANES)
    keep_mean = 1.0 - jnp.sum(mixing, axis=0)
    combined = jnp.einsum("ij,ric->rjc", transform, members, preferred_element_type=jnp.float32)
    member_mean = jnp.sum(members, axis=1, dtype=jnp.float32, keepdims=True) / MEMBERS
    mixed = (combined + member_mean * keep_mean[None, :, None]).astype(jnp.bfloat16)
    mixed = mixed.reshape(depth, mem, local, LANES).transpose(1, 0, 2, 3)
    mixed = exchange(mixed, "mem").reshape(halves, tiles, depth, local, LANES)
    analysis = mixed.transpose(3, 0, 2, 1, 4).reshape(ensemble.shape)
    return (analysis, prior_gram, posterior_gram)


def solution(mesh):
    def body(*args):
        return per_device(mesh.shape["mem"], mesh.shape["space"], *args)

    split = P(None, ("parts", "space"))
    whole = P("mem", None, ("parts", "space"))
    parts = P("parts", None)
    return jax.shard_map(
        body, mesh=mesh, in_specs=(whole, parts, P(), split), out_specs=(whole, parts, parts),
        check_vma=False,
    )
```

```python
import jax
import jax.numpy as jnp
from jax import lax
from jax.sharding import Mesh
from jax.sharding import PartitionSpec as P


MEMBERS = 64
LANES = 128
HIGHEST = lax.Precision.HIGHEST


def exchange(array, axis):
    return lax.all_to_all(array, axis, split_axis=0, concat_axis=0, tiled=True)


def per_device(mem, ensemble, transform, obs_operator, obs_weight):
    local, variables, cells = ensemble.shape
    quantities = obs_operator.shape[0]
    mixing = transform.astype(jnp.float32)
    width = cells // mem
    halves = LANES // width
    depth = variables // halves

    blocks = ensemble.reshape(local, halves, depth, mem, width)
    blocks = blocks.transpose(3, 2, 0, 1, 4).reshape(mem, depth, local, LANES)
    members = exchange(blocks, "mem")

    members = members.transpose(1, 0, 2, 3).reshape(depth, MEMBERS, LANES)
    keep_mean = 1.0 - jnp.sum(mixing, axis=0)
    combined = jnp.einsum("ij,ric->rjc", transform, members, preferred_element_type=jnp.float32)
    member_mean = jnp.sum(members, axis=1, dtype=jnp.float32, keepdims=True) / MEMBERS
    mixed = (combined + member_mean * keep_mean[None, :, None]).astype(jnp.bfloat16)
    mixed = mixed.reshape(depth, mem, local, LANES).transpose(1, 0, 2, 3)
    mixed = exchange(mixed, "mem")

    own_weights = lax.dynamic_slice_in_dim(obs_weight, lax.axis_index("mem") * width, width, 1)
    coefficient = obs_operator.astype(jnp.float32).reshape(quantities, halves, depth)
    coefficient = jnp.repeat(coefficient.transpose(0, 2, 1), width, axis=2)
    observed = jnp.sum(coefficient[:, :, None, :] * members.astype(jnp.float32)[None], axis=1)
    observed = jnp.sum(observed.reshape(quantities, MEMBERS, halves, width), axis=2)
    departures = observed - jnp.sum(observed, axis=1, keepdims=True) / MEMBERS
    partial = jnp.einsum(
        "oic,ojc->ij", departures * own_weights[:, None, :], departures, precision=HIGHEST
    )
    weight_sum = jnp.sum(own_weights)
    packed = jnp.concatenate([partial[: MEMBERS // 2], partial[MEMBERS // 2 :]], axis=1)
    packed = jnp.concatenate([packed, jnp.broadcast_to(weight_sum, (8, LANES))], axis=0)
    packed = lax.psum(packed, "space_0")
    packed = lax.psum(packed, "space_1")
    packed = exchange(jnp.broadcast_to(packed[None], (mem, *packed.shape)), "mem")
    packed = jnp.sum(packed, axis=0)
    gram_sum = jnp.concatenate([packed[:32, :MEMBERS], packed[:32, MEMBERS:]], axis=0)
    prior_gram = gram_sum / packed[32:33, :1]
    carried = jnp.dot(mixing.T, prior_gram, precision=HIGHEST)
    posterior_gram = jnp.dot(carried, mixing, precision=HIGHEST)

    mixed = mixed.reshape(mem, depth, local, halves, width)
    analysis = mixed.transpose(2, 3, 1, 0, 4).reshape(ensemble.shape)
    return (analysis, prior_gram, posterior_gram)


def solution(mesh):
    parts, mem, space = mesh.shape["parts"], mesh.shape["mem"], mesh.shape["space"]
    finer = Mesh(
        mesh.devices.reshape(parts, mem, space // 2, 2), ("parts", "mem", "space_0", "space_1")
    )

    def body(*args):
        return per_device(mem, *args)

    columns = ("parts", "space_0", "space_1")
    whole, rows, split = P("mem", None, columns), P("parts", None), P(None, columns)
    return jax.shard_map(
        body, mesh=finer, in_specs=(whole, rows, P(), split), out_specs=(whole, rows, rows),
        check_vma=False,
    )
```

```python
import functools

import jax
import jax.numpy as jnp
from jax import lax
from jax.experimental import pallas as pl
from jax.experimental.pallas import tpu as pltpu
from jax.sharding import Mesh
from jax.sharding import PartitionSpec as P


MEMBERS = 64
LANES = 128
GROUP = 4
VMEM_LIMIT = 12 << 20
HIGHEST = lax.Precision.HIGHEST


SMEM = pl.BlockSpec(memory_space=pltpu.SMEM)
VMEM = pl.BlockSpec(memory_space=pltpu.VMEM)


def exchange(array, axis):
    return lax.all_to_all(array, axis, split_axis=0, concat_axis=0, tiled=True)


def to_partner(array):
    return lax.ppermute(array, "space_1", [(0, 1), (1, 0)])


def vmem(shape, dtype):
    return jax.ShapeDtypeStruct(shape, dtype)


def kernel(body, out_shape, in_specs, flops, moved, scratch=()):
    many = isinstance(out_shape, tuple)
    return pl.pallas_call(
        body, out_shape=out_shape, in_specs=in_specs,
        out_specs=(VMEM,) * len(out_shape) if many else VMEM, scratch_shapes=scratch,
        cost_estimate=pl.CostEstimate(flops=flops, bytes_accessed=moved, transcendentals=0),
        compiler_params=pltpu.CompilerParams(vmem_limit_bytes=VMEM_LIMIT),
    )


def pack_kernel(x_ref, o_ref):
    depth, half = o_ref.shape[1], LANES // 2
    for tile in range(x_ref.shape[2] // LANES):
        at = slice(tile * LANES, (tile + 1) * LANES)
        low, high = x_ref[:depth, :, at], x_ref[depth:, :, at]
        o_ref[2 * tile] = jnp.concatenate([low[..., :half], high[..., :half]], axis=-1)
        o_ref[2 * tile + 1] = jnp.concatenate([low[..., half:], high[..., half:]], axis=-1)


def unpack_kernel(x_ref, o_ref):
    depth, half = x_ref.shape[1], LANES // 2
    for tile in range(o_ref.shape[2] // LANES):
        at = slice(tile * LANES, (tile + 1) * LANES)
        left, right = x_ref[2 * tile], x_ref[2 * tile + 1]
        o_ref[:depth, :, at] = jnp.concatenate([left[..., :half], right[..., :half]], axis=-1)
        o_ref[depth:, :, at] = jnp.concatenate([left[..., half:], right[..., half:]], axis=-1)


def fold(array, rows):
    return jnp.concatenate(
        [array[i * rows : (i + 1) * rows] for i in range(array.shape[0] // rows)], axis=1
    )


def unfold(array, width):
    return jnp.concatenate(
        [array[:, i * width : (i + 1) * width] for i in range(LANES // width)], axis=0
    )


def prepare_kernel(
    mem_ref, operator_ref, weight_ref, transform_ref,
    factor_ref, pairs_ref, total_ref, mixing_ref, turned_ref,
):
    depth, quantities, _ = factor_ref.shape
    low = lax.broadcasted_iota(jnp.int32, (quantities, LANES), 1) < LANES // 2
    operator = operator_ref[...].astype(jnp.float32)
    for r in range(depth):
        factor_ref[r] = jnp.where(low, operator[:, r : r + 1], operator[:, depth + r : depth + r + 1])
    place = mem_ref[0, 0]
    tile = weight_ref[:, pl.ds(pl.multiple_of(place // 2 * LANES, LANES), LANES)]
    turned = pltpu.roll(tile, LANES // 2, 1)
    even = place % 2 == 0
    near, far = jnp.where(even, tile, turned), jnp.where(even, turned, tile)
    for pair in range(quantities // 2):
        one, two = near[2 * pair : 2 * pair + 1], far[2 * pair + 1 : 2 * pair + 2]
        pairs_ref[pair : pair + 1, :] = jnp.where(low[:1], one, two)
    total_ref[...] = jnp.full(total_ref.shape, jnp.sum(weight_ref[...]), jnp.float32)
    mixing = transform_ref[...].astype(jnp.float32)
    mixing_ref[...] = mixing
    turned_ref[...] = mixing.T


def gram_kernel(core_ref, x_ref, factor_ref, weight_ref, total_ref, mine_ref, other_ref, lhs, rhs):
    depth, quantities = factor_ref.shape[:2]
    low = lax.broadcasted_iota(jnp.int32, (MEMBERS, LANES), 1) < LANES // 2
    zero = jnp.zeros((MEMBERS, LANES), jnp.float32)
    for first in range(0, quantities, GROUP):

        def step(r, sums, first=first):
            x = x_ref[r].astype(jnp.float32)
            return tuple(
                s + x * factor_ref[r, pl.ds(first + i, 1), :] for i, s in enumerate(sums)
            )

        sums = lax.fori_loop(0, depth, step, (zero,) * GROUP, unroll=5)
        for i in range(0, GROUP, 2):
            one, two = sums[i], sums[i + 1]
            both = jnp.where(low, one, two) + pltpu.roll(jnp.where(low, two, one), LANES // 2, 1)
            departures = both - jnp.sum(both, axis=0, keepdims=True) / MEMBERS
            pair = (first + i) // 2
            at = slice(pair * LANES, (pair + 1) * LANES)
            rhs[:, at] = departures
            lhs[:, at] = departures * weight_ref[pair : pair + 1, :]
    gram = lax.dot_general(
        lhs[...], rhs[...], (((1,), (1,)), ((), ())), precision=HIGHEST,
        preferred_element_type=jnp.float32,
    )
    half, quarter = MEMBERS // 2, MEMBERS // 4
    cross = gram[:half, half:]
    weights = total_ref[:4]
    upper = jnp.concatenate(
        [fold(gram[:half, :half], 8), fold(cross[:quarter], 4), weights], axis=0
    )
    lower = jnp.concatenate(
        [fold(gram[half:, half:], 8), fold(cross[quarter:], 4), weights], axis=0
    )
    first_core = core_ref[0, 0] == 0
    mine_ref[...] = jnp.where(first_core, upper, lower)
    other_ref[...] = jnp.where(first_core, lower, upper)


def final_kernel(core_ref, mine_ref, other_ref, mixing_ref, turned_ref, prior_ref, posterior_ref):
    half = MEMBERS // 2
    first_core = core_ref[0, 0] == 0
    mine, other = mine_ref[...], other_ref[...]
    upper, lower = jnp.where(first_core, mine, other), jnp.where(first_core, other, mine)
    cross = jnp.concatenate([unfold(upper[8:], half), unfold(lower[8:], half)], axis=0)
    gram = jnp.concatenate(
        [
            jnp.concatenate([unfold(upper[:8], half), cross], axis=1),
            jnp.concatenate([cross.T, unfold(lower[:8], half)], axis=1),
        ],
        axis=0,
    )
    prior_ref[...] = gram
    dot = functools.partial(jnp.dot, precision=HIGHEST, preferred_element_type=jnp.float32)
    posterior_ref[...] = dot(dot(turned_ref[...], gram), mixing_ref[...])


def per_device(mem, ensemble, transform, obs_operator, obs_weight):
    local, variables, cells = ensemble.shape
    quantities = obs_operator.shape[0]
    halves = LANES * mem // cells
    depth = variables // halves
    core = lax.axis_index("space_1").astype(jnp.int32).reshape(1, 1)
    place = lax.axis_index("mem").astype(jnp.int32).reshape(1, 1)
    state_bytes = 2 * ensemble.size
    square = vmem((MEMBERS, MEMBERS), jnp.float32)

    blocks = kernel(
        pack_kernel, vmem((mem, depth, local, LANES), jnp.bfloat16), [VMEM],
        state_bytes, 2 * state_bytes,
    )(ensemble.transpose(1, 0, 2))
    members = exchange(blocks, "mem")

    shapes = ((depth, quantities, LANES), (quantities // halves, LANES), (8, LANES))
    factor, pairs, total, mixing, turned = kernel(
        prepare_kernel, (*(vmem(s, jnp.float32) for s in shapes), square, square),
        [SMEM, VMEM, VMEM, VMEM], 4 * obs_weight.size, 8 * obs_weight.size,
    )(place, obs_operator, obs_weight, transform)

    members = members.transpose(1, 0, 2, 3).reshape(depth, MEMBERS, LANES)
    keep_mean = 1.0 - jnp.sum(mixing, axis=0)
    combined = jnp.einsum("ij,ric->rjc", transform, members, preferred_element_type=jnp.float32)
    member_mean = jnp.sum(members, axis=1, dtype=jnp.float32, keepdims=True) / MEMBERS
    mixed = (combined + member_mean * keep_mean[None, :, None]).astype(jnp.bfloat16)
    mixed = mixed.reshape(depth, mem, local, LANES).transpose(1, 0, 2, 3)
    mixed = exchange(mixed, "mem")

    mine, other = kernel(
        gram_kernel, (vmem((16, LANES), jnp.float32),) * 2,
        [SMEM, VMEM, VMEM, VMEM, VMEM], 4 * depth * quantities * MEMBERS * LANES, state_bytes,
        [pltpu.VMEM((MEMBERS, quantities // halves * LANES), jnp.float32)] * 2,
    )(core, members, factor, pairs, total)
    mine = mine + to_partner(other)
    mine = lax.psum(mine, "space_0")
    mine = (mine[:12] / mine[12:13]).reshape(3, 4, LANES)
    mine = exchange(jnp.broadcast_to(mine[None], (mem, *mine.shape)), "mem")
    mine = jnp.sum(mine, axis=0).reshape(12, LANES)
    other = to_partner(mine)
    prior_gram, posterior_gram = kernel(
        final_kernel, (square, square), [SMEM, VMEM, VMEM, VMEM, VMEM],
        4 * MEMBERS**3, 16 * MEMBERS**2,
    )(core, mine, other, mixing, turned)

    analysis = kernel(
        unpack_kernel, vmem((variables, local, cells), jnp.bfloat16), [VMEM],
        state_bytes, 2 * state_bytes,
    )(mixed)
    return (analysis.transpose(1, 0, 2), prior_gram, posterior_gram)


def solution(mesh):
    parts, mem, space = mesh.shape["parts"], mesh.shape["mem"], mesh.shape["space"]
    finer = Mesh(
        mesh.devices.reshape(parts, mem, space // 2, 2), ("parts", "mem", "space_0", "space_1")
    )

    def body(*args):
        return per_device(mem, *args)

    columns = ("parts", "space_0", "space_1")
    whole, rows, split = P("mem", None, columns), P("parts", None), P(None, columns)
    return jax.shard_map(
        body, mesh=finer, in_specs=(whole, rows, P(), split), out_specs=(whole, rows, rows),
        check_vma=False,
    )
```

```python
import functools

import jax
import jax.numpy as jnp
from jax import lax
from jax.experimental import pallas as pl
from jax.experimental.pallas import tpu as pltpu
from jax.sharding import Mesh
from jax.sharding import PartitionSpec as P


MEMBERS = 64
LANES = 128
GROUP = 4
BLOCK = 16
PACK_TILES = 2
GRAM_ROWS = 20
VMEM_LIMIT = 12 << 20
HIGHEST = lax.Precision.HIGHEST


SMEM = pl.BlockSpec(memory_space=pltpu.SMEM)
VMEM = pl.BlockSpec(memory_space=pltpu.VMEM)


def exchange(array, axis):
    return lax.all_to_all(array, axis, split_axis=0, concat_axis=0, tiled=True)


def vmem(shape, dtype):
    return jax.ShapeDtypeStruct(shape, dtype)


def kernel(body, out_shape, in_specs, flops, moved, scratch=(), out_specs=None, **more):
    many = isinstance(out_shape, tuple)
    return pl.pallas_call(
        body, out_shape=out_shape, in_specs=in_specs, scratch_shapes=scratch,
        out_specs=out_specs or ((VMEM,) * len(out_shape) if many else VMEM),
        cost_estimate=pl.CostEstimate(flops=flops, bytes_accessed=moved, transcendentals=0),
        **{"compiler_params": pltpu.CompilerParams(vmem_limit_bytes=VMEM_LIMIT), **more},
    )


def pack_kernel(x_ref, o_ref):
    depth, half = o_ref.shape[1], LANES // 2
    for tile in range(x_ref.shape[2] // LANES):
        at = slice(tile * LANES, (tile + 1) * LANES)
        low, high = x_ref[:depth, :, at], x_ref[depth:, :, at]
        o_ref[2 * tile] = jnp.concatenate([low[..., :half], high[..., :half]], axis=-1)
        o_ref[2 * tile + 1] = jnp.concatenate([low[..., half:], high[..., half:]], axis=-1)


def unpack_kernel(x_ref, o_ref):
    depth, half = x_ref.shape[1], LANES // 2
    for tile in range(o_ref.shape[2] // LANES):
        at = slice(tile * LANES, (tile + 1) * LANES)
        left, right = x_ref[2 * tile], x_ref[2 * tile + 1]
        o_ref[:depth, :, at] = jnp.concatenate([left[..., :half], right[..., :half]], axis=-1)
        o_ref[depth:, :, at] = jnp.concatenate([left[..., half:], right[..., half:]], axis=-1)


def fold(gram):
    rows = [gram[at : at + BLOCK, at:] for at in range(0, MEMBERS, BLOCK)]
    first = jnp.concatenate([rows[0], rows[1], rows[3]], axis=1)
    rest = jnp.concatenate([rows[2][i : i + 4] for i in range(0, BLOCK, 4)], axis=1)
    return jnp.concatenate([first, rest], axis=0)


def unfold(first, rest):
    width = 2 * BLOCK
    third = jnp.concatenate([rest[:, i : i + width] for i in range(0, LANES, width)], axis=0)
    rows = [first[:, :64], first[:, 64:112], third, first[:, 112:]]
    upper = jnp.concatenate(
        [
            jnp.concatenate([jnp.zeros((BLOCK, MEMBERS - r.shape[1]), jnp.float32), r], axis=1)
            if r.shape[1] < MEMBERS else r
            for r in rows
        ],
        axis=0,
    )
    row = lax.broadcasted_iota(jnp.int32, upper.shape, 0) // BLOCK
    column = lax.broadcasted_iota(jnp.int32, upper.shape, 1) // BLOCK
    return jnp.where(row <= column, upper, upper.T)


def prepare_kernel(
    mem_ref, operator_ref, weight_ref, transform_ref,
    factor_ref, pairs_ref, total_ref, mixing_ref, turned_ref,
):
    depth, quantities, _ = factor_ref.shape
    low = lax.broadcasted_iota(jnp.int32, (quantities, LANES), 1) < LANES // 2
    operator = operator_ref[...].astype(jnp.float32)
    for r in range(depth):
        factor_ref[r] = jnp.where(low, operator[:, r : r + 1], operator[:, depth + r : depth + r + 1])
    place = mem_ref[0, 0]
    tile = weight_ref[:, pl.ds(pl.multiple_of(place // 2 * LANES, LANES), LANES)]
    turned = pltpu.roll(tile, LANES // 2, 1)
    even = place % 2 == 0
    near, far = jnp.where(even, tile, turned), jnp.where(even, turned, tile)
    for pair in range(quantities // 2):
        one, two = near[2 * pair : 2 * pair + 1], far[2 * pair + 1 : 2 * pair + 2]
        pairs_ref[pair : pair + 1, :] = jnp.where(low[:1], one, two)
    total_ref[...] = jnp.full(total_ref.shape, jnp.sum(weight_ref[...]), jnp.float32)
    mixing = transform_ref[...].astype(jnp.float32)
    mixing_ref[...] = mixing
    turned_ref[...] = mixing.T


def gram_kernel(x_ref, factor_ref, weight_ref, total_ref, gram_ref, lhs, rhs):
    depth, quantities = factor_ref.shape[:2]
    low = lax.broadcasted_iota(jnp.int32, (MEMBERS, LANES), 1) < LANES // 2
    zero = jnp.zeros((MEMBERS, LANES), jnp.float32)
    for first in range(0, quantities, GROUP):

        def step(r, sums, first=first):
            x = x_ref[r].astype(jnp.float32)
            return tuple(
                s + x * factor_ref[r, pl.ds(first + i, 1), :] for i, s in enumerate(sums)
            )

        sums = lax.fori_loop(0, depth, step, (zero,) * GROUP, unroll=5)
        for i in range(0, GROUP, 2):
            one, two = sums[i], sums[i + 1]
            both = jnp.where(low, one, two) + pltpu.roll(jnp.where(low, two, one), LANES // 2, 1)
            departures = both - jnp.sum(both, axis=0, keepdims=True) / MEMBERS
            pair = (first + i) // 2
            at = slice(pair * LANES, (pair + 1) * LANES)
            rhs[:, at] = departures
            lhs[:, at] = departures * weight_ref[pair : pair + 1, :]
    gram = lax.dot_general(
        lhs[...], rhs[...], (((1,), (1,)), ((), ())), precision=HIGHEST,
        preferred_element_type=jnp.float32,
    )
    gram_ref[...] = jnp.concatenate([fold(gram), total_ref[:4]], axis=0)


def spread_kernel(gram_ref, o_ref):
    scaled = gram_ref[:GRAM_ROWS] / gram_ref[GRAM_ROWS : GRAM_ROWS + 1]
    for i in range(o_ref.shape[1]):
        piece = scaled[4 * i : 4 * i + 4]
        o_ref[:, i] = jnp.broadcast_to(piece[None], (o_ref.shape[0], *piece.shape))


def final_kernel(gram_ref, mixing_ref, turned_ref, prior_ref, posterior_ref):
    pieces = [jnp.sum(gram_ref[:, i], axis=0) for i in range(gram_ref.shape[1])]
    gram = unfold(jnp.concatenate(pieces[:4], axis=0), pieces[4])
    prior_ref[...] = gram
    dot = functools.partial(jnp.dot, precision=HIGHEST, preferred_element_type=jnp.float32)
    posterior_ref[...] = dot(dot(turned_ref[...], gram), mixing_ref[...])


def per_device(mem, ensemble, transform, obs_operator, obs_weight):
    local, variables, cells = ensemble.shape
    quantities = obs_operator.shape[0]
    halves = LANES * mem // cells
    depth = variables // halves
    place = lax.axis_index("mem").astype(jnp.int32).reshape(1, 1)
    state_bytes = 2 * ensemble.size
    square = vmem((MEMBERS, MEMBERS), jnp.float32)

    step = PACK_TILES * LANES
    blocks = kernel(
        pack_kernel, vmem((mem, depth, local, LANES), jnp.bfloat16),
        [pl.BlockSpec((variables, local, step), lambda i: (0, 0, i))],
        state_bytes, 2 * state_bytes, grid=(cells // step,),
        out_specs=pl.BlockSpec((2 * PACK_TILES, depth, local, LANES), lambda i: (i, 0, 0, 0)),
        compiler_params=pltpu.CompilerParams(),
    )(ensemble.transpose(1, 0, 2))
    members = exchange(blocks, "mem")

    shapes = ((depth, quantities, LANES), (quantities // halves, LANES), (8, LANES))
    factor, pairs, total, mixing, turned = kernel(
        prepare_kernel, (*(vmem(s, jnp.float32) for s in shapes), square, square),
        [SMEM, VMEM, VMEM, VMEM], 4 * obs_weight.size, 8 * obs_weight.size,
    )(place, obs_operator, obs_weight, transform)

    members = members.transpose(1, 0, 2, 3).reshape(depth, MEMBERS, LANES)
    keep_mean = 1.0 - jnp.sum(mixing, axis=0)
    combined = jnp.einsum("ij,ric->rjc", transform, members, preferred_element_type=jnp.float32)
    member_mean = jnp.sum(members, axis=1, dtype=jnp.float32, keepdims=True) / MEMBERS
    mixed = (combined + member_mean * keep_mean[None, :, None]).astype(jnp.bfloat16)
    mixed = mixed.reshape(depth, mem, local, LANES).transpose(1, 0, 2, 3)
    mixed = exchange(mixed, "mem")

    gram = kernel(
        gram_kernel, vmem((GRAM_ROWS + 4, LANES), jnp.float32), [VMEM] * 4,
        4 * depth * quantities * MEMBERS * LANES, state_bytes,
        [pltpu.VMEM((MEMBERS, quantities // halves * LANES), jnp.float32)] * 2,
    )(members, factor, pairs, total)
    gram = lax.psum(lax.psum(gram, "space_1"), "space_0")
    gram = kernel(
        spread_kernel, vmem((mem, GRAM_ROWS // 4, 4, LANES), jnp.float32),
        [VMEM], GRAM_ROWS * LANES, 4 * mem * GRAM_ROWS * LANES,
    )(gram)
    gram = exchange(gram, "mem")
    prior_gram, posterior_gram = kernel(
        final_kernel, (square, square), [VMEM] * 3, 4 * MEMBERS**3, 16 * MEMBERS**2
    )(gram, mixing, turned)

    analysis = kernel(
        unpack_kernel, vmem((variables, local, cells), jnp.bfloat16), [VMEM],
        state_bytes, 2 * state_bytes,
    )(mixed)
    return (analysis.transpose(1, 0, 2), prior_gram, posterior_gram)


def solution(mesh):
    parts, mem, space = mesh.shape["parts"], mesh.shape["mem"], mesh.shape["space"]
    finer = Mesh(
        mesh.devices.reshape(parts, mem, space // 2, 2), ("parts", "mem", "space_0", "space_1")
    )

    def body(*args):
        return per_device(mem, *args)

    columns = ("parts", "space_0", "space_1")
    whole, rows, split = P("mem", None, columns), P("parts", None), P(None, columns)
    return jax.shard_map(
        body, mesh=finer, in_specs=(whole, rows, P(), split), out_specs=(whole, rows, rows),
        check_vma=False,
    )
```

```python
import functools

import jax
import jax.numpy as jnp
from jax import lax
from jax.experimental import pallas as pl
from jax.experimental.pallas import tpu as pltpu
from jax.sharding import Mesh
from jax.sharding import PartitionSpec as P


MEMBERS = 64
LANES = 128
GROUP = 4
BLOCK = 16
PACK_STEPS = 2
VMEM_LIMIT = 12 << 20
HIGHEST = lax.Precision.HIGHEST


SMEM = pl.BlockSpec(memory_space=pltpu.SMEM)
VMEM = pl.BlockSpec(memory_space=pltpu.VMEM)
ANY = pl.BlockSpec(memory_space=pl.ANY)


def exchange(array, axis):
    return lax.all_to_all(array, axis, split_axis=0, concat_axis=0, tiled=True)


def to_partner(array):
    return lax.ppermute(array, "space_1", [(0, 1), (1, 0)])


def vmem(shape, dtype):
    return jax.ShapeDtypeStruct(shape, dtype)


def kernel(body, out_shape, in_specs, flops, moved, scratch=(), out_specs=None, **more):
    many = isinstance(out_shape, tuple)
    return pl.pallas_call(
        body, out_shape=out_shape, in_specs=in_specs, scratch_shapes=scratch,
        out_specs=out_specs or ((VMEM,) * len(out_shape) if many else VMEM),
        cost_estimate=pl.CostEstimate(flops=flops, bytes_accessed=moved, transcendentals=0),
        **{"compiler_params": pltpu.CompilerParams(vmem_limit_bytes=VMEM_LIMIT), **more},
    )


def pack_kernel(x_ref, o_ref, x, o, in_sems, out_sems):
    depth, half = o_ref.shape[1], LANES // 2
    cuts = [depth * i // PACK_STEPS for i in range(PACK_STEPS + 1)]
    steps = [slice(a, b) for a, b in zip(cuts[:-1], cuts[1:], strict=True)]
    shifted = [slice(depth + s.start, depth + s.stop) for s in steps]
    reads = [
        [pltpu.make_async_copy(x_ref.at[s], x.at[s], in_sems.at[i, j]) for j, s in enumerate(both)]
        for i, both in enumerate(zip(steps, shifted, strict=True))
    ]
    writes = [
        pltpu.make_async_copy(o.at[:, s], o_ref.at[:, s], out_sems.at[i])
        for i, s in enumerate(steps)
    ]
    for read in reads:
        read[0].start()
        read[1].start()
    for read, write, near, far in zip(reads, writes, steps, shifted, strict=True):
        read[0].wait()
        read[1].wait()
        for tile in range(x.shape[2] // LANES):
            at = slice(tile * LANES, (tile + 1) * LANES)
            low, high = x[near, :, at], x[far, :, at]
            o[2 * tile, near] = jnp.concatenate([low[..., :half], high[..., :half]], axis=-1)
            o[2 * tile + 1, near] = jnp.concatenate([low[..., half:], high[..., half:]], axis=-1)
        write.start()
    for write in writes:
        write.wait()


def unpack_kernel(x_ref, o_ref):
    depth, half = x_ref.shape[1], LANES // 2
    for tile in range(o_ref.shape[2] // LANES):
        at = slice(tile * LANES, (tile + 1) * LANES)
        left, right = x_ref[2 * tile], x_ref[2 * tile + 1]
        o_ref[:depth, :, at] = jnp.concatenate([left[..., :half], right[..., :half]], axis=-1)
        o_ref[depth:, :, at] = jnp.concatenate([left[..., half:], right[..., half:]], axis=-1)


def fold(gram):
    rows = [gram[at : at + BLOCK, at:] for at in range(0, MEMBERS, BLOCK)]
    first = jnp.concatenate([rows[0], rows[1], rows[3]], axis=1)
    rest = jnp.concatenate([rows[2][i : i + 4] for i in range(0, BLOCK, 4)], axis=1)
    return first, rest


def unfold(first, rest):
    width = 2 * BLOCK
    third = jnp.concatenate([rest[:, i : i + width] for i in range(0, LANES, width)], axis=0)
    rows = [first[:, :64], first[:, 64:112], third, first[:, 112:]]
    upper = jnp.concatenate(
        [
            jnp.concatenate([jnp.zeros((BLOCK, MEMBERS - r.shape[1]), jnp.float32), r], axis=1)
            if r.shape[1] < MEMBERS else r
            for r in rows
        ],
        axis=0,
    )
    row = lax.broadcasted_iota(jnp.int32, upper.shape, 0) // BLOCK
    column = lax.broadcasted_iota(jnp.int32, upper.shape, 1) // BLOCK
    return jnp.where(row <= column, upper, upper.T)


def prepare_kernel(
    mem_ref, operator_ref, weight_ref, transform_ref,
    factor_ref, pairs_ref, total_ref, mixing_ref, turned_ref,
):
    depth, quantities, _ = factor_ref.shape
    low = lax.broadcasted_iota(jnp.int32, (quantities, LANES), 1) < LANES // 2
    operator = operator_ref[...].astype(jnp.float32)
    for r in range(depth):
        factor_ref[r] = jnp.where(low, operator[:, r : r + 1], operator[:, depth + r : depth + r + 1])
    place = mem_ref[0, 0]
    tile = weight_ref[:, pl.ds(pl.multiple_of(place // 2 * LANES, LANES), LANES)]
    turned = pltpu.roll(tile, LANES // 2, 1)
    even = place % 2 == 0
    near, far = jnp.where(even, tile, turned), jnp.where(even, turned, tile)
    for pair in range(quantities // 2):
        one, two = near[2 * pair : 2 * pair + 1], far[2 * pair + 1 : 2 * pair + 2]
        pairs_ref[pair : pair + 1, :] = jnp.where(low[:1], one, two)
    total_ref[...] = jnp.full(total_ref.shape, jnp.sum(weight_ref[...]), jnp.float32)
    mixing = transform_ref[...].astype(jnp.float32)
    mixing_ref[...] = mixing
    turned_ref[...] = mixing.T


def gram_kernel(core_ref, x_ref, factor_ref, weight_ref, total_ref, mine_ref, other_ref, lhs, rhs):
    depth, quantities = factor_ref.shape[:2]
    low = lax.broadcasted_iota(jnp.int32, (MEMBERS, LANES), 1) < LANES // 2
    zero = jnp.zeros((MEMBERS, LANES), jnp.float32)
    for first in range(0, quantities, GROUP):

        def step(r, sums, first=first):
            x = x_ref[r].astype(jnp.float32)
            return tuple(
                s + x * factor_ref[r, pl.ds(first + i, 1), :] for i, s in enumerate(sums)
            )

        sums = lax.fori_loop(0, depth, step, (zero,) * GROUP, unroll=5)
        for i in range(0, GROUP, 2):
            one, two = sums[i], sums[i + 1]
            both = jnp.where(low, one, two) + pltpu.roll(jnp.where(low, two, one), LANES // 2, 1)
            departures = both - jnp.sum(both, axis=0, keepdims=True) / MEMBERS
            pair = (first + i) // 2
            at = slice(pair * LANES, (pair + 1) * LANES)
            rhs[:, at] = departures
            lhs[:, at] = departures * weight_ref[pair : pair + 1, :]
    gram = lax.dot_general(
        lhs[...], rhs[...], (((1,), (1,)), ((), ())), precision=HIGHEST,
        preferred_element_type=jnp.float32,
    )
    first, rest = fold(gram)
    halves = [
        (first[8 * i : 8 * i + 4], first[8 * i + 4 : 8 * i + 8],
         jnp.concatenate([rest[2 * i : 2 * i + 2], total_ref[:2]], axis=0))
        for i in range(2)
    ]
    first_core = core_ref[0, 0] == 0
    for i, (upper, lower) in enumerate(zip(*halves, strict=True)):
        mine_ref[i] = jnp.where(first_core, upper, lower)
        other_ref[i] = jnp.where(first_core, lower, upper)


def spread_kernel(core_ref, mine_ref, other_ref, o_ref):
    first_core = core_ref[0, 0] == 0
    mine, other = mine_ref[...], other_ref[...]
    total = mine[2, 2:3]
    upper, lower = jnp.where(first_core, mine, other), jnp.where(first_core, other, mine)
    rest = jnp.concatenate([upper[2, :2], lower[2, :2]], axis=0)
    for i, piece in enumerate((upper[0], upper[1], lower[0], lower[1], rest)):
        o_ref[:, i] = jnp.broadcast_to((piece / total)[None], (o_ref.shape[0], *piece.shape))


def final_kernel(gram_ref, mixing_ref, turned_ref, prior_ref, posterior_ref):
    pieces = [jnp.sum(gram_ref[:, i], axis=0) for i in range(gram_ref.shape[1])]
    gram = unfold(jnp.concatenate(pieces[:4], axis=0), pieces[4])
    prior_ref[...] = gram
    dot = functools.partial(jnp.dot, precision=HIGHEST, preferred_element_type=jnp.float32)
    posterior_ref[...] = dot(dot(turned_ref[...], gram), mixing_ref[...])


def per_device(mem, ensemble, transform, obs_operator, obs_weight):
    local, variables, cells = ensemble.shape
    quantities = obs_operator.shape[0]
    halves = LANES * mem // cells
    depth = variables // halves
    core = lax.axis_index("space_1").astype(jnp.int32).reshape(1, 1)
    place = lax.axis_index("mem").astype(jnp.int32).reshape(1, 1)
    state_bytes = 2 * ensemble.size
    square = vmem((MEMBERS, MEMBERS), jnp.float32)

    block_shape, state_shape = (mem, depth, local, LANES), (variables, local, cells)
    blocks = kernel(
        pack_kernel, vmem(block_shape, jnp.bfloat16), [ANY],
        state_bytes, 2 * state_bytes,
        [
            pltpu.VMEM(state_shape, jnp.bfloat16), pltpu.VMEM(block_shape, jnp.bfloat16),
            pltpu.SemaphoreType.DMA((PACK_STEPS, 2)), pltpu.SemaphoreType.DMA((PACK_STEPS,)),
        ],
        out_specs=ANY, compiler_params=pltpu.CompilerParams(),
    )(ensemble.transpose(1, 0, 2))
    members = exchange(blocks, "mem")

    shapes = ((depth, quantities, LANES), (quantities // halves, LANES), (8, LANES))
    factor, pairs, total, mixing, turned = kernel(
        prepare_kernel, (*(vmem(s, jnp.float32) for s in shapes), square, square),
        [SMEM, VMEM, VMEM, VMEM], 4 * obs_weight.size, 8 * obs_weight.size,
    )(place, obs_operator, obs_weight, transform)

    members = members.transpose(1, 0, 2, 3).reshape(depth, MEMBERS, LANES)
    keep_mean = 1.0 - jnp.sum(mixing, axis=0)
    combined = jnp.einsum("ij,ric->rjc", transform, members, preferred_element_type=jnp.float32)
    member_mean = jnp.sum(members, axis=1, dtype=jnp.float32, keepdims=True) / MEMBERS
    mixed = (combined + member_mean * keep_mean[None, :, None]).astype(jnp.bfloat16)
    mixed = mixed.reshape(depth, mem, local, LANES).transpose(1, 0, 2, 3)
    mixed = exchange(mixed, "mem")

    half = (3, 4, LANES)
    mine, other = kernel(
        gram_kernel, (vmem(half, jnp.float32),) * 2, [SMEM, *[VMEM] * 4],
        4 * depth * quantities * MEMBERS * LANES, state_bytes,
        [pltpu.VMEM((MEMBERS, quantities // halves * LANES), jnp.float32)] * 2,
    )(core, members, factor, pairs, total)
    mine = lax.psum(mine + to_partner(other), "space_0")
    other = to_partner(mine)
    gram = kernel(
        spread_kernel, vmem((mem, 5, 4, LANES), jnp.float32),
        [SMEM, VMEM, VMEM], MEMBERS**2, 4 * mem * MEMBERS**2,
    )(core, mine, other)
    gram = exchange(gram, "mem")
    prior_gram, posterior_gram = kernel(
        final_kernel, (square, square), [VMEM] * 3, 4 * MEMBERS**3, 16 * MEMBERS**2
    )(gram, mixing, turned)

    analysis = kernel(
        unpack_kernel, vmem((variables, local, cells), jnp.bfloat16), [VMEM],
        state_bytes, 2 * state_bytes,
    )(mixed)
    return (analysis.transpose(1, 0, 2), prior_gram, posterior_gram)


def solution(mesh):
    parts, mem, space = mesh.shape["parts"], mesh.shape["mem"], mesh.shape["space"]
    finer = Mesh(
        mesh.devices.reshape(parts, mem, space // 2, 2), ("parts", "mem", "space_0", "space_1")
    )

    def body(*args):
        return per_device(mem, *args)

    columns = ("parts", "space_0", "space_1")
    whole, rows, split = P("mem", None, columns), P("parts", None), P(None, columns)
    return jax.shard_map(
        body, mesh=finer, in_specs=(whole, rows, P(), split), out_specs=(whole, rows, rows),
        check_vma=False,
    )
```

```python
import functools

import jax
import jax.numpy as jnp
from jax import lax
from jax.experimental import pallas as pl
from jax.experimental.pallas import tpu as pltpu
from jax.sharding import Mesh
from jax.sharding import PartitionSpec as P


MEMBERS = 64
LANES = 128
GROUP = 4
BLOCK = 4
PACK_STEPS = 5
VMEM_LIMIT = 12 << 20
HIGHEST = lax.Precision.HIGHEST


SMEM = pl.BlockSpec(memory_space=pltpu.SMEM)
VMEM = pl.BlockSpec(memory_space=pltpu.VMEM)
ANY = pl.BlockSpec(memory_space=pl.ANY)


def exchange(array, axis, groups=None):
    return lax.all_to_all(
        array, axis, split_axis=0, concat_axis=0, tiled=True, axis_index_groups=groups
    )


def to_partner(array):
    return lax.ppermute(array, "space_1", [(0, 1), (1, 0)])


def vmem(shape, dtype):
    return jax.ShapeDtypeStruct(shape, dtype)


def kernel(body, out_shape, in_specs, flops, moved, scratch=(), out_specs=None, **more):
    many = isinstance(out_shape, tuple)
    return pl.pallas_call(
        body, out_shape=out_shape, in_specs=in_specs, scratch_shapes=scratch,
        out_specs=out_specs or ((VMEM,) * len(out_shape) if many else VMEM),
        cost_estimate=pl.CostEstimate(flops=flops, bytes_accessed=moved, transcendentals=0),
        **{"compiler_params": pltpu.CompilerParams(vmem_limit_bytes=VMEM_LIMIT), **more},
    )


def pack_kernel(x_ref, o_ref, x, o, in_sems, out_sems):
    depth, half = o_ref.shape[1], LANES // 2
    cuts = [depth * i // PACK_STEPS for i in range(PACK_STEPS + 1)]
    steps = [slice(a, b) for a, b in zip(cuts[:-1], cuts[1:], strict=True)]
    shifted = [slice(depth + s.start, depth + s.stop) for s in steps]
    reads = [
        [pltpu.make_async_copy(x_ref.at[s], x.at[s], in_sems.at[i, j]) for j, s in enumerate(both)]
        for i, both in enumerate(zip(steps, shifted, strict=True))
    ]
    writes = [
        pltpu.make_async_copy(o.at[:, s], o_ref.at[:, s], out_sems.at[i])
        for i, s in enumerate(steps)
    ]
    for read in reads:
        read[0].start()
        read[1].start()
    for read, write, near, far in zip(reads, writes, steps, shifted, strict=True):
        read[0].wait()
        read[1].wait()
        for tile in range(x.shape[2] // LANES):
            at = slice(tile * LANES, (tile + 1) * LANES)
            low, high = x[near, :, at], x[far, :, at]
            o[2 * tile, near] = jnp.concatenate([low[..., :half], high[..., :half]], axis=-1)
            o[2 * tile + 1, near] = jnp.concatenate([low[..., half:], high[..., half:]], axis=-1)
        write.start()
    for write in writes:
        write.wait()


def unpack_kernel(x_ref, o_ref):
    depth, half = x_ref.shape[1], LANES // 2
    for tile in range(o_ref.shape[2] // LANES):
        at = slice(tile * LANES, (tile + 1) * LANES)
        left, right = x_ref[2 * tile], x_ref[2 * tile + 1]
        o_ref[:depth, :, at] = jnp.concatenate([left[..., :half], right[..., :half]], axis=-1)
        o_ref[depth:, :, at] = jnp.concatenate([left[..., half:], right[..., half:]], axis=-1)


TILES = ((0, 1, 15), (2, 3, 11), (4, 5, 7), (6, 8, 9, 12, 13))
REST = (10, 14)


def fold(gram):
    def tile(rows):
        at = [BLOCK * r for r in rows]
        return jnp.concatenate([gram[a : a + BLOCK, a:] for a in at], axis=1)

    rest = tile(REST)
    row = jnp.concatenate([rest[i : i + 1] for i in range(BLOCK)], axis=1)
    return [tile(rows) for rows in TILES], row


def unfold(tiles, row):
    width = LANES // BLOCK
    rest = jnp.concatenate([row[:, i * width : (i + 1) * width] for i in range(BLOCK)], axis=0)
    rows = {}
    for members, tile in zip((*TILES, REST), (*tiles, rest), strict=True):
        start = 0
        for b in members:
            wide = MEMBERS - BLOCK * b
            piece = tile[:, start : start + wide]
            if wide < MEMBERS:
                blank = jnp.zeros((BLOCK, MEMBERS - wide), jnp.float32)
                piece = jnp.concatenate([blank, piece], axis=1)
            rows[b] = piece
            start += wide
    upper = jnp.concatenate([rows[b] for b in sorted(rows)], axis=0)
    row = lax.broadcasted_iota(jnp.int32, upper.shape, 0) // BLOCK
    column = lax.broadcasted_iota(jnp.int32, upper.shape, 1) // BLOCK
    return jnp.where(row <= column, upper, upper.T)


def prepare_kernel(
    mem_ref, operator_ref, weight_ref, transform_ref,
    factor_ref, pairs_ref, total_ref, mixing_ref, turned_ref,
):
    depth, quantities, _ = factor_ref.shape
    low = lax.broadcasted_iota(jnp.int32, (quantities, LANES), 1) < LANES // 2
    operator = operator_ref[...].astype(jnp.float32)
    for r in range(depth):
        factor_ref[r] = jnp.where(low, operator[:, r : r + 1], operator[:, depth + r : depth + r + 1])
    place = mem_ref[0, 0]
    tile = weight_ref[:, pl.ds(pl.multiple_of(place // 2 * LANES, LANES), LANES)]
    turned = pltpu.roll(tile, LANES // 2, 1)
    even = place % 2 == 0
    near, far = jnp.where(even, tile, turned), jnp.where(even, turned, tile)
    for pair in range(quantities // 2):
        one, two = near[2 * pair : 2 * pair + 1], far[2 * pair + 1 : 2 * pair + 2]
        pairs_ref[pair : pair + 1, :] = jnp.where(low[:1], one, two)
    total_ref[...] = jnp.full(total_ref.shape, jnp.sum(weight_ref[...]), jnp.float32)
    mixing = transform_ref[...].astype(jnp.float32)
    mixing_ref[...] = mixing
    turned_ref[...] = mixing.T


def gram_kernel(core_ref, x_ref, factor_ref, weight_ref, total_ref, mine_ref, other_ref, lhs, rhs):
    depth, quantities = factor_ref.shape[:2]
    low = lax.broadcasted_iota(jnp.int32, (MEMBERS, LANES), 1) < LANES // 2
    zero = jnp.zeros((MEMBERS, LANES), jnp.float32)
    for first in range(0, quantities, GROUP):

        def step(r, sums, first=first):
            x = x_ref[r].astype(jnp.float32)
            return tuple(
                s + x * factor_ref[r, pl.ds(first + i, 1), :] for i, s in enumerate(sums)
            )

        sums = lax.fori_loop(0, depth, step, (zero,) * GROUP, unroll=5)
        for i in range(0, GROUP, 2):
            one, two = sums[i], sums[i + 1]
            both = jnp.where(low, one, two) + pltpu.roll(jnp.where(low, two, one), LANES // 2, 1)
            departures = both - jnp.sum(both, axis=0, keepdims=True) / MEMBERS
            pair = (first + i) // 2
            at = slice(pair * LANES, (pair + 1) * LANES)
            rhs[:, at] = departures
            lhs[:, at] = departures * weight_ref[pair : pair + 1, :]
    gram = lax.dot_general(
        lhs[...], rhs[...], (((1,), (1,)), ((), ())), precision=HIGHEST,
        preferred_element_type=jnp.float32,
    )
    tiles, row = fold(gram)
    halves = [
        (*tiles[:2], total_ref[:4]),
        (*tiles[2:], jnp.concatenate([total_ref[:2], row, row], axis=0)),
    ]
    first_core = core_ref[0, 0] == 0
    for i, (upper, lower) in enumerate(zip(*halves, strict=True)):
        mine_ref[i] = jnp.where(first_core, upper, lower)
        other_ref[i] = jnp.where(first_core, lower, upper)


def spread_kernel(core_ref, mine_ref, other_ref, o_ref):
    first_core = core_ref[0, 0] == 0
    mine, other = mine_ref[...], other_ref[...]
    total = mine[2, :1]
    upper, lower = jnp.where(first_core, mine, other), jnp.where(first_core, other, mine)
    tiles = (upper[0], upper[1], lower[0], lower[1], lower[2, 2:3])
    rows = [(t / total)[i : i + 1] for t in tiles for i in range(t.shape[0])]
    for i, row in enumerate(rows):
        o_ref[:, i] = jnp.broadcast_to(row[None], (o_ref.shape[0], 1, LANES))


def final_kernel(gram_ref, mixing_ref, turned_ref, prior_ref, posterior_ref):
    rows = jnp.sum(gram_ref[...], axis=0)
    tiles = [
        jnp.concatenate([rows[BLOCK * i + k] for k in range(BLOCK)], axis=0)
        for i in range(len(TILES))
    ]
    gram = unfold(tiles, rows[BLOCK * len(TILES)])
    prior_ref[...] = gram
    dot = functools.partial(jnp.dot, precision=HIGHEST, preferred_element_type=jnp.float32)
    posterior_ref[...] = dot(dot(turned_ref[...], gram), mixing_ref[...])


def per_device(mem, ensemble, transform, obs_operator, obs_weight):
    local, variables, cells = ensemble.shape
    quantities = obs_operator.shape[0]
    halves = LANES * mem // cells
    depth = variables // halves
    core = lax.axis_index("space_1").astype(jnp.int32).reshape(1, 1)
    place = lax.axis_index("mem").astype(jnp.int32).reshape(1, 1)
    state_bytes = 2 * ensemble.size
    square = vmem((MEMBERS, MEMBERS), jnp.float32)

    block_shape, state_shape = (mem, depth, local, LANES), (variables, local, cells)
    blocks = kernel(
        pack_kernel, vmem(block_shape, jnp.bfloat16), [ANY],
        state_bytes, 2 * state_bytes,
        [
            pltpu.VMEM(state_shape, jnp.bfloat16), pltpu.VMEM(block_shape, jnp.bfloat16),
            pltpu.SemaphoreType.DMA((PACK_STEPS, 2)), pltpu.SemaphoreType.DMA((PACK_STEPS,)),
        ],
        out_specs=ANY, compiler_params=pltpu.CompilerParams(),
    )(ensemble.transpose(1, 0, 2))
    members = exchange(blocks, "mem")

    shapes = ((depth, quantities, LANES), (quantities // halves, LANES), (8, LANES))
    factor, pairs, total, mixing, turned = kernel(
        prepare_kernel, (*(vmem(s, jnp.float32) for s in shapes), square, square),
        [SMEM, VMEM, VMEM, VMEM], 4 * obs_weight.size, 8 * obs_weight.size,
    )(place, obs_operator, obs_weight, transform)

    members = members.transpose(1, 0, 2, 3).reshape(depth, MEMBERS, LANES)
    keep_mean = 1.0 - jnp.sum(mixing, axis=0)
    combined = jnp.einsum("ij,ric->rjc", transform, members, preferred_element_type=jnp.float32)
    member_mean = jnp.sum(members, axis=1, dtype=jnp.float32, keepdims=True) / MEMBERS
    mixed = (combined + member_mean * keep_mean[None, :, None]).astype(jnp.bfloat16)
    mixed = mixed.reshape(depth, mem, local, LANES).transpose(1, 0, 2, 3)
    mixed = exchange(mixed, "mem")

    half = (3, 4, LANES)
    mine, other = kernel(
        gram_kernel, (vmem(half, jnp.float32),) * 2, [SMEM, *[VMEM] * 4],
        4 * depth * quantities * MEMBERS * LANES, state_bytes,
        [pltpu.VMEM((MEMBERS, quantities // halves * LANES), jnp.float32)] * 2,
    )(core, members, factor, pairs, total)
    mine = lax.psum(mine + to_partner(other), "space_0")
    other = to_partner(mine)
    gram = kernel(
        spread_kernel, vmem((mem, 17, 1, LANES), jnp.float32),
        [SMEM, VMEM, VMEM], MEMBERS**2, 4 * mem * MEMBERS**2,
    )(core, mine, other)
    far_first = [i // 2 + i % 2 * (mem // 2) for i in range(mem)]
    gram = exchange(gram, "mem", [far_first])
    prior_gram, posterior_gram = kernel(
        final_kernel, (square, square), [VMEM] * 3, 4 * MEMBERS**3, 16 * MEMBERS**2
    )(gram, mixing, turned)

    analysis = kernel(
        unpack_kernel, vmem((variables, local, cells), jnp.bfloat16), [VMEM],
        state_bytes, 2 * state_bytes,
    )(mixed)
    return (analysis.transpose(1, 0, 2), prior_gram, posterior_gram)


def solution(mesh):
    parts, mem, space = mesh.shape["parts"], mesh.shape["mem"], mesh.shape["space"]
    finer = Mesh(
        mesh.devices.reshape(parts, mem, space // 2, 2), ("parts", "mem", "space_0", "space_1")
    )

    def body(*args):
        return per_device(mem, *args)

    columns = ("parts", "space_0", "space_1")
    whole, rows, split = P("mem", None, columns), P("parts", None), P(None, columns)
    return jax.shard_map(
        body, mesh=finer, in_specs=(whole, rows, P(), split), out_specs=(whole, rows, rows),
        check_vma=False,
    )
```

```python
import functools

import jax
import jax.numpy as jnp
from jax import lax
from jax.experimental import pallas as pl
from jax.experimental.pallas import tpu as pltpu
from jax.sharding import Mesh
from jax.sharding import PartitionSpec as P


MEMBERS = 64
LANES = 128
GROUP = 4
BLOCK = 16
PACK_STEPS = 2
VMEM_LIMIT = 12 << 20
HIGHEST = lax.Precision.HIGHEST


SMEM = pl.BlockSpec(memory_space=pltpu.SMEM)
VMEM = pl.BlockSpec(memory_space=pltpu.VMEM)
ANY = pl.BlockSpec(memory_space=pl.ANY)


def exchange(array, axis, groups=None):
    return lax.all_to_all(
        array, axis, split_axis=0, concat_axis=0, tiled=True, axis_index_groups=groups
    )


def vmem(shape, dtype):
    return jax.ShapeDtypeStruct(shape, dtype)


def kernel(body, out_shape, in_specs, flops, moved, scratch=(), out_specs=None, **more):
    many = isinstance(out_shape, tuple)
    return pl.pallas_call(
        body, out_shape=out_shape, in_specs=in_specs, scratch_shapes=scratch,
        out_specs=out_specs or ((VMEM,) * len(out_shape) if many else VMEM),
        cost_estimate=pl.CostEstimate(flops=flops, bytes_accessed=moved, transcendentals=0),
        **{"compiler_params": pltpu.CompilerParams(vmem_limit_bytes=VMEM_LIMIT), **more},
    )


def pack_kernel(x_ref, o_ref, x, o, in_sems, out_sems):
    depth, half = o_ref.shape[1], LANES // 2
    cuts = [depth * i // PACK_STEPS for i in range(PACK_STEPS + 1)]
    steps = [slice(a, b) for a, b in zip(cuts[:-1], cuts[1:], strict=True)]
    shifted = [slice(depth + s.start, depth + s.stop) for s in steps]
    reads = [
        [pltpu.make_async_copy(x_ref.at[s], x.at[s], in_sems.at[i, j]) for j, s in enumerate(both)]
        for i, both in enumerate(zip(steps, shifted, strict=True))
    ]
    writes = [
        pltpu.make_async_copy(o.at[:, s], o_ref.at[:, s], out_sems.at[i])
        for i, s in enumerate(steps)
    ]
    for read in reads:
        read[0].start()
        read[1].start()
    for read, write, near, far in zip(reads, writes, steps, shifted, strict=True):
        read[0].wait()
        read[1].wait()
        for tile in range(x.shape[2] // LANES):
            at = slice(tile * LANES, (tile + 1) * LANES)
            low, high = x[near, :, at], x[far, :, at]
            o[2 * tile, near] = jnp.concatenate([low[..., :half], high[..., :half]], axis=-1)
            o[2 * tile + 1, near] = jnp.concatenate([low[..., half:], high[..., half:]], axis=-1)
        write.start()
    for write in writes:
        write.wait()


def unpack_kernel(x_ref, o_ref):
    depth, half = x_ref.shape[1], LANES // 2
    for tile in range(o_ref.shape[2] // LANES):
        at = slice(tile * LANES, (tile + 1) * LANES)
        left, right = x_ref[2 * tile], x_ref[2 * tile + 1]
        o_ref[:depth, :, at] = jnp.concatenate([left[..., :half], right[..., :half]], axis=-1)
        o_ref[depth:, :, at] = jnp.concatenate([left[..., half:], right[..., half:]], axis=-1)


def fold(gram, total):
    row = lax.broadcasted_iota(jnp.int32, (BLOCK, BLOCK), 0)
    column = lax.broadcasted_iota(jnp.int32, (BLOCK, BLOCK), 1)
    starts = range(0, MEMBERS, BLOCK)
    across = [gram[a : a + BLOCK, a + BLOCK :] for a in starts[:-1]]
    inner = [gram[a : a + BLOCK, a : a + BLOCK] for a in starts]
    pairs = [
        jnp.where(row < column, one, jnp.where(row > column, two, total))
        for one, two in zip(inner[::2], inner[1::2], strict=True)
    ]
    return jnp.concatenate([*across, *pairs], axis=1)


def unfold(packed):
    row = lax.broadcasted_iota(jnp.int32, (BLOCK, BLOCK), 0)
    column = lax.broadcasted_iota(jnp.int32, (BLOCK, BLOCK), 1)
    blocks = MEMBERS // BLOCK
    start, rows = 0, []
    pair_start = BLOCK * blocks * (blocks - 1) // 2
    for b in range(blocks):
        wide = MEMBERS - BLOCK * (b + 1)
        at = pair_start + BLOCK * (b // 2)
        pair = packed[:, at : at + BLOCK]
        pieces = [jnp.where(row < column if b % 2 == 0 else row > column, pair, 0.0)]
        if b:
            pieces.insert(0, jnp.zeros((BLOCK, BLOCK * b), jnp.float32))
        if wide:
            pieces.append(packed[:, start : start + wide])
        rows.append(jnp.concatenate(pieces, axis=1))
        start += wide
    half = jnp.concatenate(rows, axis=0)
    gram = half + half.T
    row = lax.broadcasted_iota(jnp.int32, gram.shape, 0)
    column = lax.broadcasted_iota(jnp.int32, gram.shape, 1)
    return jnp.where(row == column, -jnp.sum(gram, axis=1, keepdims=True), gram)


def prepare_kernel(
    mem_ref, operator_ref, weight_ref, transform_ref,
    factor_ref, pairs_ref, total_ref, mixing_ref, turned_ref,
):
    depth, quantities, _ = factor_ref.shape
    low = lax.broadcasted_iota(jnp.int32, (quantities, LANES), 1) < LANES // 2
    operator = operator_ref[...].astype(jnp.float32)
    for r in range(depth):
        factor_ref[r] = jnp.where(low, operator[:, r : r + 1], operator[:, depth + r : depth + r + 1])
    place = mem_ref[0, 0]
    tile = weight_ref[:, pl.ds(pl.multiple_of(place // 2 * LANES, LANES), LANES)]
    turned = pltpu.roll(tile, LANES // 2, 1)
    even = place % 2 == 0
    near, far = jnp.where(even, tile, turned), jnp.where(even, turned, tile)
    for pair in range(quantities // 2):
        one, two = near[2 * pair : 2 * pair + 1], far[2 * pair + 1 : 2 * pair + 2]
        pairs_ref[pair : pair + 1, :] = jnp.where(low[:1], one, two)
    total_ref[...] = jnp.full(total_ref.shape, jnp.sum(weight_ref[...]), jnp.float32)
    mixing = transform_ref[...].astype(jnp.float32)
    mixing_ref[...] = mixing
    turned_ref[...] = mixing.T


def gram_kernel(x_ref, factor_ref, weight_ref, total_ref, gram_ref, lhs, rhs):
    depth, quantities = factor_ref.shape[:2]
    low = lax.broadcasted_iota(jnp.int32, (MEMBERS, LANES), 1) < LANES // 2
    zero = jnp.zeros((MEMBERS, LANES), jnp.float32)
    for first in range(0, quantities, GROUP):

        def step(r, sums, first=first):
            x = x_ref[r].astype(jnp.float32)
            return tuple(
                s + x * factor_ref[r, pl.ds(first + i, 1), :] for i, s in enumerate(sums)
            )

        sums = lax.fori_loop(0, depth, step, (zero,) * GROUP, unroll=5)
        for i in range(0, GROUP, 2):
            one, two = sums[i], sums[i + 1]
            both = jnp.where(low, one, two) + pltpu.roll(jnp.where(low, two, one), LANES // 2, 1)
            departures = both - jnp.sum(both, axis=0, keepdims=True) / MEMBERS
            pair = (first + i) // 2
            at = slice(pair * LANES, (pair + 1) * LANES)
            rhs[:, at] = departures
            lhs[:, at] = departures * weight_ref[pair : pair + 1, :]
    gram = lax.dot_general(
        lhs[...], rhs[...], (((1,), (1,)), ((), ())), precision=HIGHEST,
        preferred_element_type=jnp.float32,
    )
    gram_ref[...] = fold(gram, total_ref[:1, :1])


def spread_kernel(gram_ref, o_ref):
    first = LANES - MEMBERS // 2
    scaled = gram_ref[...] / gram_ref[:1, first : first + 1]
    for i in range(BLOCK // 4):
        piece = scaled[4 * i : 4 * i + 4]
        o_ref[:, i] = jnp.broadcast_to(piece[None], (o_ref.shape[0], *piece.shape))


def final_kernel(gram_ref, mixing_ref, turned_ref, prior_ref, posterior_ref):
    pieces = [jnp.sum(gram_ref[:, i], axis=0) for i in range(gram_ref.shape[1])]
    gram = unfold(jnp.concatenate(pieces, axis=0))
    prior_ref[...] = gram
    dot = functools.partial(jnp.dot, precision=HIGHEST, preferred_element_type=jnp.float32)
    posterior_ref[...] = dot(dot(turned_ref[...], gram), mixing_ref[...])


def per_device(mem, ensemble, transform, obs_operator, obs_weight):
    local, variables, cells = ensemble.shape
    quantities = obs_operator.shape[0]
    halves = LANES * mem // cells
    depth = variables // halves
    place = lax.axis_index("mem").astype(jnp.int32).reshape(1, 1)
    state_bytes = 2 * ensemble.size
    square = vmem((MEMBERS, MEMBERS), jnp.float32)

    block_shape, state_shape = (mem, depth, local, LANES), (variables, local, cells)
    blocks = kernel(
        pack_kernel, vmem(block_shape, jnp.bfloat16), [ANY],
        state_bytes, 2 * state_bytes,
        [
            pltpu.VMEM(state_shape, jnp.bfloat16), pltpu.VMEM(block_shape, jnp.bfloat16),
            pltpu.SemaphoreType.DMA((PACK_STEPS, 2)), pltpu.SemaphoreType.DMA((PACK_STEPS,)),
        ],
        out_specs=ANY, compiler_params=pltpu.CompilerParams(),
    )(ensemble.transpose(1, 0, 2))
    members = exchange(blocks, "mem")

    shapes = ((depth, quantities, LANES), (quantities // halves, LANES), (8, LANES))
    factor, pairs, total, mixing, turned = kernel(
        prepare_kernel, (*(vmem(s, jnp.float32) for s in shapes), square, square),
        [SMEM, VMEM, VMEM, VMEM], 4 * obs_weight.size, 8 * obs_weight.size,
    )(place, obs_operator, obs_weight, transform)

    members = members.transpose(1, 0, 2, 3).reshape(depth, MEMBERS, LANES)
    keep_mean = 1.0 - jnp.sum(mixing, axis=0)
    combined = jnp.einsum("ij,ric->rjc", transform, members, preferred_element_type=jnp.float32)
    member_mean = jnp.sum(members, axis=1, dtype=jnp.float32, keepdims=True) / MEMBERS
    mixed = (combined + member_mean * keep_mean[None, :, None]).astype(jnp.bfloat16)
    mixed = mixed.reshape(depth, mem, local, LANES).transpose(1, 0, 2, 3)
    mixed = exchange(mixed, "mem")

    gram = kernel(
        gram_kernel, vmem((BLOCK, LANES), jnp.float32), [VMEM] * 4,
        4 * depth * quantities * MEMBERS * LANES, state_bytes,
        [pltpu.VMEM((MEMBERS, quantities // halves * LANES), jnp.float32)] * 2,
    )(members, factor, pairs, total)
    gram = lax.psum(lax.psum(gram, "space_1"), "space_0")
    gram = kernel(
        spread_kernel, vmem((mem, BLOCK // 4, 4, LANES), jnp.float32), [VMEM],
        MEMBERS**2, 2 * mem * MEMBERS**2,
    )(gram)
    far_first = [i // 2 + i % 2 * (mem // 2) for i in range(mem)]
    gram = exchange(gram, "mem", [far_first])
    prior_gram, posterior_gram = kernel(
        final_kernel, (square, square), [VMEM] * 3, 4 * MEMBERS**3, 16 * MEMBERS**2
    )(gram, mixing, turned)

    analysis = kernel(
        unpack_kernel, vmem((variables, local, cells), jnp.bfloat16), [VMEM],
        state_bytes, 2 * state_bytes,
    )(mixed)
    return (analysis.transpose(1, 0, 2), prior_gram, posterior_gram)


def solution(mesh):
    parts, mem, space = mesh.shape["parts"], mesh.shape["mem"], mesh.shape["space"]
    finer = Mesh(
        mesh.devices.reshape(parts, mem, space // 2, 2), ("parts", "mem", "space_0", "space_1")
    )

    def body(*args):
        return per_device(mem, *args)

    columns = ("parts", "space_0", "space_1")
    whole, rows, split = P("mem", None, columns), P("parts", None), P(None, columns)
    return jax.shard_map(
        body, mesh=finer, in_specs=(whole, rows, P(), split), out_specs=(whole, rows, rows),
        check_vma=False,
    )
```

```python
import functools

import jax
import jax.numpy as jnp
from jax import lax
from jax.experimental import pallas as pl
from jax.experimental.pallas import tpu as pltpu
from jax.sharding import Mesh
from jax.sharding import PartitionSpec as P


MEMBERS = 64
LANES = 128
GROUP = 4
BLOCK = 16
PACK_STEPS = 2
VMEM_LIMIT = 12 << 20
HIGHEST = lax.Precision.HIGHEST


SMEM = pl.BlockSpec(memory_space=pltpu.SMEM)
VMEM = pl.BlockSpec(memory_space=pltpu.VMEM)
ANY = pl.BlockSpec(memory_space=pl.ANY)
HBM = pl.BlockSpec(memory_space=pltpu.HBM)


def exchange(array, axis, groups=None):
    return lax.all_to_all(
        array, axis, split_axis=0, concat_axis=0, tiled=True, axis_index_groups=groups
    )


def in_hbm(array):
    return pltpu.with_memory_space_constraint(array, pltpu.HBM)


def vmem(shape, dtype):
    return jax.ShapeDtypeStruct(shape, dtype)


def kernel(body, out_shape, in_specs, flops, moved, scratch=(), out_specs=None, **more):
    many = isinstance(out_shape, tuple)
    return pl.pallas_call(
        body, out_shape=out_shape, in_specs=in_specs, scratch_shapes=scratch,
        out_specs=out_specs or ((VMEM,) * len(out_shape) if many else VMEM),
        cost_estimate=pl.CostEstimate(flops=flops, bytes_accessed=moved, transcendentals=0),
        **{"compiler_params": pltpu.CompilerParams(vmem_limit_bytes=VMEM_LIMIT), **more},
    )


def pack_kernel(x_ref, transform_ref, o_ref, keep_ref, mixing_ref, x, sems, sem):
    depth, half = o_ref.shape[1], LANES // 2
    cuts = [depth * i // PACK_STEPS for i in range(PACK_STEPS + 1)]
    steps = [slice(a, b) for a, b in zip(cuts[:-1], cuts[1:], strict=True)]
    shifted = [slice(depth + s.start, depth + s.stop) for s in steps]
    reads = [
        [pltpu.make_async_copy(x_ref.at[s], x.at[s], sems.at[i, j]) for j, s in enumerate(both)]
        for i, both in enumerate(zip(steps, shifted, strict=True))
    ]
    mixing_read = pltpu.make_async_copy(transform_ref, mixing_ref, sem)
    for near_read, far_read in reads:
        near_read.start()
        far_read.start()
    mixing_read.start()
    for (near_read, far_read), near, far in zip(reads, steps, shifted, strict=True):
        near_read.wait()
        far_read.wait()
        for tile in range(x.shape[2] // LANES):
            at = slice(tile * LANES, (tile + 1) * LANES)
            low, high = x[near, :, at], x[far, :, at]
            o_ref[2 * tile, near] = jnp.concatenate([low[..., :half], high[..., :half]], axis=-1)
            o_ref[2 * tile + 1, near] = jnp.concatenate([low[..., half:], high[..., half:]], axis=-1)
    mixing_read.wait()
    turned = mixing_ref[...].astype(jnp.float32).T
    keep = (1.0 - jnp.sum(turned, axis=1, keepdims=True)) / MEMBERS
    keep_ref[...] = jnp.broadcast_to(keep, keep_ref.shape)


def fold(gram, total):
    row = lax.broadcasted_iota(jnp.int32, (BLOCK, BLOCK), 0)
    column = lax.broadcasted_iota(jnp.int32, (BLOCK, BLOCK), 1)
    starts = range(0, MEMBERS, BLOCK)
    across = [gram[a : a + BLOCK, a + BLOCK :] for a in starts[:-1]]
    inner = [gram[a : a + BLOCK, a : a + BLOCK] for a in starts]
    pairs = [
        jnp.where(row < column, one, jnp.where(row > column, two, total))
        for one, two in zip(inner[::2], inner[1::2], strict=True)
    ]
    return jnp.concatenate([*across, *pairs], axis=1)


def unfold(packed):
    row = lax.broadcasted_iota(jnp.int32, (BLOCK, BLOCK), 0)
    column = lax.broadcasted_iota(jnp.int32, (BLOCK, BLOCK), 1)
    blocks = MEMBERS // BLOCK
    start, rows = 0, []
    pair_start = BLOCK * blocks * (blocks - 1) // 2
    for b in range(blocks):
        wide = MEMBERS - BLOCK * (b + 1)
        at = pair_start + BLOCK * (b // 2)
        pair = packed[:, at : at + BLOCK]
        pieces = [jnp.where(row < column if b % 2 == 0 else row > column, pair, 0.0)]
        if b:
            pieces.insert(0, jnp.zeros((BLOCK, BLOCK * b), jnp.float32))
        if wide:
            pieces.append(packed[:, start : start + wide])
        rows.append(jnp.concatenate(pieces, axis=1))
        start += wide
    half = jnp.concatenate(rows, axis=0)
    gram = half + half.T
    row = lax.broadcasted_iota(jnp.int32, gram.shape, 0)
    column = lax.broadcasted_iota(jnp.int32, gram.shape, 1)
    return jnp.where(row == column, -jnp.sum(gram, axis=1, keepdims=True), gram)


def prepare_kernel(
    mem_ref, operator_ref, weight_ref, transform_ref,
    factor_ref, pairs_ref, total_ref, mixing_ref, turned_ref,
):
    depth, quantities, _ = factor_ref.shape
    low = lax.broadcasted_iota(jnp.int32, (quantities, LANES), 1) < LANES // 2
    operator = operator_ref[...].astype(jnp.float32)
    for r in range(depth):
        factor_ref[r] = jnp.where(low, operator[:, r : r + 1], operator[:, depth + r : depth + r + 1])
    place = mem_ref[0, 0]
    tile = weight_ref[:, pl.ds(pl.multiple_of(place // 2 * LANES, LANES), LANES)]
    turned = pltpu.roll(tile, LANES // 2, 1)
    even = place % 2 == 0
    near, far = jnp.where(even, tile, turned), jnp.where(even, turned, tile)
    for pair in range(quantities // 2):
        one, two = near[2 * pair : 2 * pair + 1], far[2 * pair + 1 : 2 * pair + 2]
        pairs_ref[pair : pair + 1, :] = jnp.where(low[:1], one, two)
    total_ref[...] = jnp.full(total_ref.shape, jnp.sum(weight_ref[...]), jnp.float32)
    mixing = transform_ref[...].astype(jnp.float32)
    mixing_ref[...] = mixing
    turned_ref[...] = mixing.T


def gram_kernel(x_ref, factor_ref, weight_ref, total_ref, gram_ref, lhs, rhs):
    depth, quantities = factor_ref.shape[:2]
    low = lax.broadcasted_iota(jnp.int32, (MEMBERS, LANES), 1) < LANES // 2
    zero = jnp.zeros((MEMBERS, LANES), jnp.float32)
    for first in range(0, quantities, GROUP):

        def step(r, sums, first=first):
            x = x_ref[r].astype(jnp.float32)
            return tuple(
                s + x * factor_ref[r, pl.ds(first + i, 1), :] for i, s in enumerate(sums)
            )

        sums = lax.fori_loop(0, depth, step, (zero,) * GROUP, unroll=5)
        for i in range(0, GROUP, 2):
            one, two = sums[i], sums[i + 1]
            both = jnp.where(low, one, two) + pltpu.roll(jnp.where(low, two, one), LANES // 2, 1)
            departures = both - jnp.sum(both, axis=0, keepdims=True) / MEMBERS
            pair = (first + i) // 2
            at = slice(pair * LANES, (pair + 1) * LANES)
            rhs[:, at] = departures
            lhs[:, at] = departures * weight_ref[pair : pair + 1, :]
    gram = lax.dot_general(
        lhs[...], rhs[...], (((1,), (1,)), ((), ())), precision=HIGHEST,
        preferred_element_type=jnp.float32,
    )
    gram_ref[...] = fold(gram, total_ref[:1, :1])


def spread_kernel(gram_ref, o_ref):
    first = LANES - MEMBERS // 2
    scaled = gram_ref[...] / gram_ref[:1, first : first + 1]
    for i in range(BLOCK // 4):
        piece = scaled[4 * i : 4 * i + 4]
        o_ref[:, i] = jnp.broadcast_to(piece[None], (o_ref.shape[0], *piece.shape))


def final_kernel(
    x_ref, gram_ref, mixing_ref, turned_ref, o_ref, prior_ref, posterior_ref, o, sem
):
    depth, half = x_ref.shape[1], LANES // 2
    for tile in range(o.shape[2] // LANES):
        at = slice(tile * LANES, (tile + 1) * LANES)
        left, right = x_ref[2 * tile], x_ref[2 * tile + 1]
        o[:depth, :, at] = jnp.concatenate([left[..., :half], right[..., :half]], axis=-1)
        o[depth:, :, at] = jnp.concatenate([left[..., half:], right[..., half:]], axis=-1)
    copy = pltpu.make_async_copy(o, o_ref, sem)
    copy.start()
    pieces = [jnp.sum(gram_ref[:, i], axis=0) for i in range(gram_ref.shape[1])]
    gram = unfold(jnp.concatenate(pieces, axis=0))
    prior_ref[...] = gram
    dot = functools.partial(jnp.dot, precision=HIGHEST, preferred_element_type=jnp.float32)
    posterior_ref[...] = dot(dot(turned_ref[...], gram), mixing_ref[...])
    copy.wait()


def per_device(mem, ensemble, transform, obs_operator, obs_weight):
    local, variables, cells = ensemble.shape
    quantities = obs_operator.shape[0]
    halves = LANES * mem // cells
    depth = variables // halves
    place = lax.axis_index("mem").astype(jnp.int32).reshape(1, 1)
    state_bytes = 2 * ensemble.size
    square = vmem((MEMBERS, MEMBERS), jnp.float32)

    shapes = (
        vmem((mem, depth, local, LANES), jnp.bfloat16), vmem((MEMBERS, LANES), jnp.float32),
        vmem(transform.shape, transform.dtype),
    )
    blocks, keep_share, mixing_here = kernel(
        pack_kernel, shapes, [HBM, HBM], state_bytes, 2 * state_bytes,
        [
            pltpu.VMEM((variables, local, cells), jnp.bfloat16),
            pltpu.SemaphoreType.DMA((PACK_STEPS, 2)), pltpu.SemaphoreType.DMA,
        ],
    )(in_hbm(ensemble.transpose(1, 0, 2)), in_hbm(transform))
    members = exchange(blocks, "mem")

    shapes = ((depth, quantities, LANES), (quantities // halves, LANES), (8, LANES))
    factor, pairs, total, mixing, turned = kernel(
        prepare_kernel, (*(vmem(s, jnp.float32) for s in shapes), square, square),
        [SMEM, VMEM, VMEM, VMEM], 4 * obs_weight.size, 8 * obs_weight.size,
    )(place, obs_operator, obs_weight, mixing_here)

    members = members.transpose(1, 0, 2, 3).reshape(depth, MEMBERS, LANES)
    combined = jnp.einsum("ij,ric->rjc", mixing_here, members, preferred_element_type=jnp.float32)
    totals = jnp.sum(members, axis=1, dtype=jnp.float32, keepdims=True)
    mixed = (combined + totals * keep_share[None]).astype(jnp.bfloat16)
    mixed = mixed.reshape(depth, mem, local, LANES).transpose(1, 0, 2, 3)
    mixed = exchange(mixed, "mem")

    gram = kernel(
        gram_kernel, vmem((BLOCK, LANES), jnp.float32), [VMEM] * 4,
        4 * depth * quantities * MEMBERS * LANES, state_bytes,
        [pltpu.VMEM((MEMBERS, quantities // halves * LANES), jnp.float32)] * 2,
    )(members, factor, pairs, total)
    gram = lax.psum(lax.psum(gram, "space_1"), "space_0")
    gram = kernel(
        spread_kernel, vmem((mem, BLOCK // 4, 4, LANES), jnp.float32), [VMEM],
        MEMBERS**2, 2 * mem * MEMBERS**2,
    )(gram)
    far_first = [i // 2 + i % 2 * (mem // 2) for i in range(mem)]
    gram = exchange(gram, "mem", [far_first])
    state = vmem((variables, local, cells), jnp.bfloat16)
    analysis, prior_gram, posterior_gram = kernel(
        final_kernel, (state, square, square), [VMEM] * 4, state_bytes,
        2 * state_bytes, [pltpu.VMEM(state.shape, state.dtype), pltpu.SemaphoreType.DMA],
        out_specs=(ANY, VMEM, VMEM),
    )(mixed, gram, mixing, turned)
    return (analysis.transpose(1, 0, 2), prior_gram, posterior_gram)


def solution(mesh):
    parts, mem, space = mesh.shape["parts"], mesh.shape["mem"], mesh.shape["space"]
    finer = Mesh(
        mesh.devices.reshape(parts, mem, space // 2, 2), ("parts", "mem", "space_0", "space_1")
    )

    def body(*args):
        return per_device(mem, *args)

    columns = ("parts", "space_0", "space_1")
    whole, rows, split = P("mem", None, columns), P("parts", None), P(None, columns)
    return jax.shard_map(
        body, mesh=finer, in_specs=(whole, rows, P(), split), out_specs=(whole, rows, rows),
        check_vma=False,
    )
```

```python
import functools

import jax
import jax.numpy as jnp
from jax import lax
from jax.experimental import pallas as pl
from jax.experimental.pallas import tpu as pltpu
from jax.sharding import Mesh
from jax.sharding import PartitionSpec as P


MEMBERS = 64
LANES = 128
GROUP = 4
BLOCK = 16
PACK_STEPS = 5
VMEM_LIMIT = 12 << 20
HIGHEST = lax.Precision.HIGHEST


SMEM = pl.BlockSpec(memory_space=pltpu.SMEM)
VMEM = pl.BlockSpec(memory_space=pltpu.VMEM)
HBM = pl.BlockSpec(memory_space=pltpu.HBM)


def exchange(array, axis, groups=None):
    return lax.all_to_all(
        array, axis, split_axis=0, concat_axis=0, tiled=True, axis_index_groups=groups
    )


def in_hbm(array):
    return pltpu.with_memory_space_constraint(array, pltpu.HBM)


def vmem(shape, dtype):
    return jax.ShapeDtypeStruct(shape, dtype)


def kernel(body, out_shape, in_specs, flops, moved, scratch=(), out_specs=None, **more):
    many = isinstance(out_shape, tuple)
    return pl.pallas_call(
        body, out_shape=out_shape, in_specs=in_specs, scratch_shapes=scratch,
        out_specs=out_specs or ((VMEM,) * len(out_shape) if many else VMEM),
        cost_estimate=pl.CostEstimate(flops=flops, bytes_accessed=moved, transcendentals=0),
        **{"compiler_params": pltpu.CompilerParams(vmem_limit_bytes=VMEM_LIMIT), **more},
    )


def pack_kernel(x_ref, transform_ref, o_ref, keep_ref, mixing_ref, x, sems, sem):
    depth, half = o_ref.shape[1], LANES // 2
    cuts = [depth * i // PACK_STEPS for i in range(PACK_STEPS + 1)]
    steps = [slice(a, b) for a, b in zip(cuts[:-1], cuts[1:], strict=True)]
    shifted = [slice(depth + s.start, depth + s.stop) for s in steps]
    reads = [
        [pltpu.make_async_copy(x_ref.at[s], x.at[s], sems.at[i, j]) for j, s in enumerate(both)]
        for i, both in enumerate(zip(steps, shifted, strict=True))
    ]
    mixing_read = pltpu.make_async_copy(transform_ref, mixing_ref, sem)
    for near_read, far_read in reads:
        near_read.start()
        far_read.start()
    mixing_read.start()
    for (near_read, far_read), near, far in zip(reads, steps, shifted, strict=True):
        near_read.wait()
        far_read.wait()
        for tile in range(x.shape[2] // LANES):
            at = slice(tile * LANES, (tile + 1) * LANES)
            low, high = x[near, :, at], x[far, :, at]
            o_ref[2 * tile, near] = jnp.concatenate([low[..., :half], high[..., :half]], axis=-1)
            o_ref[2 * tile + 1, near] = jnp.concatenate([low[..., half:], high[..., half:]], axis=-1)
    mixing_read.wait()
    turned = mixing_ref[...].astype(jnp.float32).T
    keep = (1.0 - jnp.sum(turned, axis=1, keepdims=True)) / MEMBERS
    keep_ref[...] = jnp.broadcast_to(keep, keep_ref.shape)


def unpack_kernel(x_ref, o_ref):
    depth, half = x_ref.shape[1], LANES // 2
    for tile in range(o_ref.shape[2] // LANES):
        at = slice(tile * LANES, (tile + 1) * LANES)
        left, right = x_ref[2 * tile], x_ref[2 * tile + 1]
        o_ref[:depth, :, at] = jnp.concatenate([left[..., :half], right[..., :half]], axis=-1)
        o_ref[depth:, :, at] = jnp.concatenate([left[..., half:], right[..., half:]], axis=-1)


def fold(gram, total):
    row = lax.broadcasted_iota(jnp.int32, (BLOCK, BLOCK), 0)
    column = lax.broadcasted_iota(jnp.int32, (BLOCK, BLOCK), 1)
    starts = range(0, MEMBERS, BLOCK)
    across = [gram[a : a + BLOCK, a + BLOCK :] for a in starts[:-1]]
    inner = [gram[a : a + BLOCK, a : a + BLOCK] for a in starts]
    pairs = [
        jnp.where(row < column, one, jnp.where(row > column, two, total))
        for one, two in zip(inner[::2], inner[1::2], strict=True)
    ]
    return jnp.concatenate([*across, *pairs], axis=1)


def unfold(packed):
    row = lax.broadcasted_iota(jnp.int32, (BLOCK, BLOCK), 0)
    column = lax.broadcasted_iota(jnp.int32, (BLOCK, BLOCK), 1)
    blocks = MEMBERS // BLOCK
    start, rows = 0, []
    pair_start = BLOCK * blocks * (blocks - 1) // 2
    for b in range(blocks):
        wide = MEMBERS - BLOCK * (b + 1)
        at = pair_start + BLOCK * (b // 2)
        pair = packed[:, at : at + BLOCK]
        pieces = [jnp.where(row < column if b % 2 == 0 else row > column, pair, 0.0)]
        if b:
            pieces.insert(0, jnp.zeros((BLOCK, BLOCK * b), jnp.float32))
        if wide:
            pieces.append(packed[:, start : start + wide])
        rows.append(jnp.concatenate(pieces, axis=1))
        start += wide
    half = jnp.concatenate(rows, axis=0)
    gram = half + half.T
    row = lax.broadcasted_iota(jnp.int32, gram.shape, 0)
    column = lax.broadcasted_iota(jnp.int32, gram.shape, 1)
    return jnp.where(row == column, -jnp.sum(gram, axis=1, keepdims=True), gram)


def prepare_kernel(
    mem_ref, operator_ref, weight_ref, transform_ref,
    factor_ref, pairs_ref, total_ref, mixing_ref, turned_ref,
):
    depth, quantities, _ = factor_ref.shape
    low = lax.broadcasted_iota(jnp.int32, (quantities, LANES), 1) < LANES // 2
    operator = operator_ref[...].astype(jnp.float32)
    for r in range(depth):
        factor_ref[r] = jnp.where(low, operator[:, r : r + 1], operator[:, depth + r : depth + r + 1])
    place = mem_ref[0, 0]
    tile = weight_ref[:, pl.ds(pl.multiple_of(place // 2 * LANES, LANES), LANES)]
    turned = pltpu.roll(tile, LANES // 2, 1)
    even = place % 2 == 0
    near, far = jnp.where(even, tile, turned), jnp.where(even, turned, tile)
    for pair in range(quantities // 2):
        one, two = near[2 * pair : 2 * pair + 1], far[2 * pair + 1 : 2 * pair + 2]
        pairs_ref[pair : pair + 1, :] = jnp.where(low[:1], one, two)
    total_ref[...] = jnp.full(total_ref.shape, jnp.sum(weight_ref[...]), jnp.float32)
    mixing = transform_ref[...].astype(jnp.float32)
    mixing_ref[...] = mixing
    turned_ref[...] = mixing.T


def gram_kernel(x_ref, factor_ref, weight_ref, total_ref, gram_ref, lhs, rhs):
    depth, quantities = factor_ref.shape[:2]
    low = lax.broadcasted_iota(jnp.int32, (MEMBERS, LANES), 1) < LANES // 2
    zero = jnp.zeros((MEMBERS, LANES), jnp.float32)
    for first in range(0, quantities, GROUP):

        def step(r, sums, first=first):
            x = x_ref[r].astype(jnp.float32)
            return tuple(
                s + x * factor_ref[r, pl.ds(first + i, 1), :] for i, s in enumerate(sums)
            )

        sums = lax.fori_loop(0, depth, step, (zero,) * GROUP, unroll=5)
        for i in range(0, GROUP, 2):
            one, two = sums[i], sums[i + 1]
            both = jnp.where(low, one, two) + pltpu.roll(jnp.where(low, two, one), LANES // 2, 1)
            departures = both - jnp.sum(both, axis=0, keepdims=True) / MEMBERS
            pair = (first + i) // 2
            at = slice(pair * LANES, (pair + 1) * LANES)
            rhs[:, at] = departures
            lhs[:, at] = departures * weight_ref[pair : pair + 1, :]
    gram = lax.dot_general(
        lhs[...], rhs[...], (((1,), (1,)), ((), ())), precision=HIGHEST,
        preferred_element_type=jnp.float32,
    )
    gram_ref[...] = fold(gram, total_ref[:1, :1])


def spread_kernel(gram_ref, o_ref):
    first = LANES - MEMBERS // 2
    scaled = gram_ref[...] / gram_ref[:1, first : first + 1]
    for i in range(BLOCK // 4):
        piece = scaled[4 * i : 4 * i + 4]
        o_ref[:, i] = jnp.broadcast_to(piece[None], (o_ref.shape[0], *piece.shape))


def final_kernel(gram_ref, mixing_ref, turned_ref, prior_ref, posterior_ref):
    pieces = [jnp.sum(gram_ref[:, i], axis=0) for i in range(gram_ref.shape[1])]
    gram = unfold(jnp.concatenate(pieces, axis=0))
    prior_ref[...] = gram
    dot = functools.partial(jnp.dot, precision=HIGHEST, preferred_element_type=jnp.float32)
    posterior_ref[...] = dot(dot(turned_ref[...], gram), mixing_ref[...])


def per_device(mem, ensemble, transform, obs_operator, obs_weight):
    local, variables, cells = ensemble.shape
    quantities = obs_operator.shape[0]
    halves = LANES * mem // cells
    depth = variables // halves
    place = lax.axis_index("mem").astype(jnp.int32).reshape(1, 1)
    state_bytes = 2 * ensemble.size
    square = vmem((MEMBERS, MEMBERS), jnp.float32)

    shapes = (
        vmem((mem, depth, local, LANES), jnp.bfloat16), vmem((MEMBERS, LANES), jnp.float32),
        vmem(transform.shape, transform.dtype),
    )
    blocks, keep_share, mixing_here = kernel(
        pack_kernel, shapes, [HBM, HBM], state_bytes, 2 * state_bytes,
        [
            pltpu.VMEM((variables, local, cells), jnp.bfloat16),
            pltpu.SemaphoreType.DMA((PACK_STEPS, 2)), pltpu.SemaphoreType.DMA,
        ],
    )(in_hbm(ensemble.transpose(1, 0, 2)), in_hbm(transform))
    members = exchange(blocks, "mem")

    shapes = ((depth, quantities, LANES), (quantities // halves, LANES), (8, LANES))
    factor, pairs, total, mixing, turned = kernel(
        prepare_kernel, (*(vmem(s, jnp.float32) for s in shapes), square, square),
        [SMEM, VMEM, VMEM, VMEM], 4 * obs_weight.size, 8 * obs_weight.size,
    )(place, obs_operator, obs_weight, mixing_here)

    members = members.transpose(1, 0, 2, 3).reshape(depth, MEMBERS, LANES)
    combined = jnp.einsum("ij,ric->rjc", mixing_here, members, preferred_element_type=jnp.float32)
    totals = jnp.sum(members, axis=1, dtype=jnp.float32, keepdims=True)
    mixed = (combined + totals * keep_share[None]).astype(jnp.bfloat16)
    mixed = mixed.reshape(depth, mem, local, LANES).transpose(1, 0, 2, 3)
    mixed = exchange(mixed, "mem")

    gram = kernel(
        gram_kernel, vmem((BLOCK, LANES), jnp.float32), [VMEM] * 4,
        4 * depth * quantities * MEMBERS * LANES, state_bytes,
        [pltpu.VMEM((MEMBERS, quantities // halves * LANES), jnp.float32)] * 2,
    )(members, factor, pairs, total)
    gram = lax.psum(lax.psum(gram, "space_1"), "space_0")
    gram = kernel(
        spread_kernel, vmem((mem, BLOCK // 4, 4, LANES), jnp.float32), [VMEM],
        MEMBERS**2, 2 * mem * MEMBERS**2,
    )(gram)
    far_first = [i // 2 + (i + 1) % 2 * (mem // 2) for i in range(mem)]
    gram = exchange(gram, "mem", [far_first])
    prior_gram, posterior_gram = kernel(
        final_kernel, (square, square), [VMEM] * 3, 4 * MEMBERS**3, 16 * MEMBERS**2
    )(gram, mixing, turned)

    analysis = kernel(
        unpack_kernel, vmem((variables, local, cells), jnp.bfloat16), [VMEM],
        state_bytes, 2 * state_bytes,
    )(mixed)
    return (analysis.transpose(1, 0, 2), prior_gram, posterior_gram)


def solution(mesh):
    parts, mem, space = mesh.shape["parts"], mesh.shape["mem"], mesh.shape["space"]
    finer = Mesh(
        mesh.devices.reshape(parts, mem, space // 2, 2), ("parts", "mem", "space_0", "space_1")
    )

    def body(*args):
        return per_device(mem, *args)

    columns = ("parts", "space_0", "space_1")
    whole, rows, split = P("mem", None, columns), P("parts", None), P(None, columns)
    return jax.shard_map(
        body, mesh=finer, in_specs=(whole, rows, P(), split), out_specs=(whole, rows, rows),
        check_vma=False,
    )
```

```python
import functools

import jax
import jax.numpy as jnp
from jax import lax
from jax.experimental import pallas as pl
from jax.experimental.pallas import tpu as pltpu
from jax.sharding import Mesh
from jax.sharding import PartitionSpec as P


MEMBERS = 64
LANES = 128
GROUP = 4
BLOCK = 16
PACK_STEPS = 5
VMEM_LIMIT = 12 << 20
HIGHEST = lax.Precision.HIGHEST


SMEM = pl.BlockSpec(memory_space=pltpu.SMEM)
VMEM = pl.BlockSpec(memory_space=pltpu.VMEM)
HBM = pl.BlockSpec(memory_space=pltpu.HBM)


def exchange(array, axis, groups=None):
    return lax.all_to_all(
        array, axis, split_axis=0, concat_axis=0, tiled=True, axis_index_groups=groups
    )


def in_hbm(array):
    return pltpu.with_memory_space_constraint(array, pltpu.HBM)


def vmem(shape, dtype):
    return jax.ShapeDtypeStruct(shape, dtype)


def kernel(body, out_shape, in_specs, flops, moved, scratch=(), out_specs=None, **more):
    many = isinstance(out_shape, tuple)
    return pl.pallas_call(
        body, out_shape=out_shape, in_specs=in_specs, scratch_shapes=scratch,
        out_specs=out_specs or ((VMEM,) * len(out_shape) if many else VMEM),
        cost_estimate=pl.CostEstimate(flops=flops, bytes_accessed=moved, transcendentals=0),
        **{"compiler_params": pltpu.CompilerParams(vmem_limit_bytes=VMEM_LIMIT), **more},
    )


def pack_kernel(x_ref, transform_ref, o_ref, keep_ref, mixing_ref, x, sems, sem):
    depth, half = o_ref.shape[1], LANES // 2
    cuts = [depth * i // PACK_STEPS for i in range(PACK_STEPS + 1)]
    steps = [slice(a, b) for a, b in zip(cuts[:-1], cuts[1:], strict=True)]
    shifted = [slice(depth + s.start, depth + s.stop) for s in steps]
    reads = [
        [pltpu.make_async_copy(x_ref.at[s], x.at[s], sems.at[i, j]) for j, s in enumerate(both)]
        for i, both in enumerate(zip(steps, shifted, strict=True))
    ]
    mixing_read = pltpu.make_async_copy(transform_ref, mixing_ref, sem)
    for near_read, far_read in reads:
        near_read.start()
        far_read.start()
    mixing_read.start()
    for (near_read, far_read), near, far in zip(reads, steps, shifted, strict=True):
        near_read.wait()
        far_read.wait()
        for tile in range(x.shape[2] // LANES):
            at = slice(tile * LANES, (tile + 1) * LANES)
            low, high = x[near, :, at], x[far, :, at]
            o_ref[2 * tile, near] = jnp.concatenate([low[..., :half], high[..., :half]], axis=-1)
            o_ref[2 * tile + 1, near] = jnp.concatenate([low[..., half:], high[..., half:]], axis=-1)
    mixing_read.wait()
    turned = mixing_ref[...].astype(jnp.float32).T
    keep = (1.0 - jnp.sum(turned, axis=1, keepdims=True)) / MEMBERS
    keep_ref[...] = jnp.broadcast_to(keep, keep_ref.shape)


def unpack_kernel(x_ref, o_ref):
    depth, half = x_ref.shape[1], LANES // 2
    for tile in range(o_ref.shape[2] // LANES):
        at = slice(tile * LANES, (tile + 1) * LANES)
        left, right = x_ref[2 * tile], x_ref[2 * tile + 1]
        o_ref[:depth, :, at] = jnp.concatenate([left[..., :half], right[..., :half]], axis=-1)
        o_ref[depth:, :, at] = jnp.concatenate([left[..., half:], right[..., half:]], axis=-1)


def fold(gram, total):
    row = lax.broadcasted_iota(jnp.int32, (BLOCK, BLOCK), 0)
    column = lax.broadcasted_iota(jnp.int32, (BLOCK, BLOCK), 1)
    starts = range(0, MEMBERS, BLOCK)
    across = [gram[a : a + BLOCK, a + BLOCK :] for a in starts[:-1]]
    inner = [gram[a : a + BLOCK, a : a + BLOCK] for a in starts]
    pairs = [
        jnp.where(row < column, one, jnp.where(row > column, two, total))
        for one, two in zip(inner[::2], inner[1::2], strict=True)
    ]
    return jnp.concatenate([*across, *pairs], axis=1)


def unfold(packed):
    row = lax.broadcasted_iota(jnp.int32, (BLOCK, BLOCK), 0)
    column = lax.broadcasted_iota(jnp.int32, (BLOCK, BLOCK), 1)
    blocks = MEMBERS // BLOCK
    start, rows = 0, []
    pair_start = BLOCK * blocks * (blocks - 1) // 2
    for b in range(blocks):
        wide = MEMBERS - BLOCK * (b + 1)
        at = pair_start + BLOCK * (b // 2)
        pair = packed[:, at : at + BLOCK]
        pieces = [jnp.where(row < column if b % 2 == 0 else row > column, pair, 0.0)]
        if b:
            pieces.insert(0, jnp.zeros((BLOCK, BLOCK * b), jnp.float32))
        if wide:
            pieces.append(packed[:, start : start + wide])
        rows.append(jnp.concatenate(pieces, axis=1))
        start += wide
    half = jnp.concatenate(rows, axis=0)
    gram = half + half.T
    row = lax.broadcasted_iota(jnp.int32, gram.shape, 0)
    column = lax.broadcasted_iota(jnp.int32, gram.shape, 1)
    return jnp.where(row == column, -jnp.sum(gram, axis=1, keepdims=True), gram)


def prepare_kernel(
    mem_ref, operator_ref, weight_ref, transform_ref,
    factor_ref, pairs_ref, total_ref, mixing_ref, turned_ref,
):
    depth, quantities, _ = factor_ref.shape
    low = lax.broadcasted_iota(jnp.int32, (quantities, LANES), 1) < LANES // 2
    operator = operator_ref[...].astype(jnp.float32)
    for r in range(depth):
        factor_ref[r] = jnp.where(low, operator[:, r : r + 1], operator[:, depth + r : depth + r + 1])
    place = mem_ref[0, 0]
    tile = weight_ref[:, pl.ds(pl.multiple_of(place // 2 * LANES, LANES), LANES)]
    turned = pltpu.roll(tile, LANES // 2, 1)
    even = place % 2 == 0
    near, far = jnp.where(even, tile, turned), jnp.where(even, turned, tile)
    for pair in range(quantities // 2):
        one, two = near[2 * pair : 2 * pair + 1], far[2 * pair + 1 : 2 * pair + 2]
        pairs_ref[pair : pair + 1, :] = jnp.where(low[:1], one, two)
    total_ref[...] = jnp.full(total_ref.shape, jnp.sum(weight_ref[...]), jnp.float32)
    mixing = transform_ref[...].astype(jnp.float32)
    mixing_ref[...] = mixing
    turned_ref[...] = mixing.T


def gram_kernel(x_ref, factor_ref, weight_ref, total_ref, gram_ref, lhs, rhs):
    depth, quantities = factor_ref.shape[:2]
    low = lax.broadcasted_iota(jnp.int32, (MEMBERS, LANES), 1) < LANES // 2
    zero = jnp.zeros((MEMBERS, LANES), jnp.float32)
    for first in range(0, quantities, GROUP):

        def step(r, sums, first=first):
            x = x_ref[r].astype(jnp.float32)
            return tuple(
                s + x * factor_ref[r, pl.ds(first + i, 1), :] for i, s in enumerate(sums)
            )

        sums = lax.fori_loop(0, depth, step, (zero,) * GROUP, unroll=5)
        for i in range(0, GROUP, 2):
            one, two = sums[i], sums[i + 1]
            both = jnp.where(low, one, two) + pltpu.roll(jnp.where(low, two, one), LANES // 2, 1)
            departures = both - jnp.sum(both, axis=0, keepdims=True) / MEMBERS
            pair = (first + i) // 2
            at = slice(pair * LANES, (pair + 1) * LANES)
            rhs[:, at] = departures
            lhs[:, at] = departures * weight_ref[pair : pair + 1, :]
    gram = lax.dot_general(
        lhs[...], rhs[...], (((1,), (1,)), ((), ())), precision=HIGHEST,
        preferred_element_type=jnp.float32,
    )
    gram_ref[...] = fold(gram, total_ref[:1, :1])


def spread_kernel(gram_ref, o_ref):
    first = LANES - MEMBERS // 2
    scaled = gram_ref[...] / gram_ref[:1, first : first + 1]
    for i in range(BLOCK // 4):
        piece = scaled[4 * i : 4 * i + 4]
        o_ref[:, i] = jnp.broadcast_to(piece[None], (o_ref.shape[0], *piece.shape))


def final_kernel(gram_ref, mixing_ref, turned_ref, prior_ref, posterior_ref):
    pieces = [jnp.sum(gram_ref[:, i], axis=0) for i in range(gram_ref.shape[1])]
    gram = unfold(jnp.concatenate(pieces, axis=0))
    prior_ref[...] = gram
    dot = functools.partial(jnp.dot, precision=HIGHEST, preferred_element_type=jnp.float32)
    posterior_ref[...] = dot(dot(turned_ref[...], gram), mixing_ref[...])


def per_device(mem, ensemble, transform, obs_operator, obs_weight):
    local, variables, cells = ensemble.shape
    quantities = obs_operator.shape[0]
    halves = LANES * mem // cells
    depth = variables // halves
    place = lax.axis_index("mem").astype(jnp.int32).reshape(1, 1)
    state_bytes = 2 * ensemble.size
    square = vmem((MEMBERS, MEMBERS), jnp.float32)

    shapes = (
        vmem((mem, depth, local, LANES), jnp.bfloat16), vmem((MEMBERS, LANES), jnp.float32),
        vmem(transform.shape, transform.dtype),
    )
    blocks, keep_share, mixing_here = kernel(
        pack_kernel, shapes, [HBM, HBM], state_bytes, 2 * state_bytes,
        [
            pltpu.VMEM((variables, local, cells), jnp.bfloat16),
            pltpu.SemaphoreType.DMA((PACK_STEPS, 2)), pltpu.SemaphoreType.DMA,
        ],
    )(in_hbm(ensemble.transpose(1, 0, 2)), in_hbm(transform))
    members = exchange(blocks, "mem")

    shapes = ((depth, quantities, LANES), (quantities // halves, LANES), (8, LANES))
    factor, pairs, total, mixing, turned = kernel(
        prepare_kernel, (*(vmem(s, jnp.float32) for s in shapes), square, square),
        [SMEM, VMEM, VMEM, VMEM], 4 * obs_weight.size, 8 * obs_weight.size,
    )(place, obs_operator, obs_weight, mixing_here)

    members = members.transpose(1, 0, 2, 3).reshape(depth, MEMBERS, LANES)
    combined = jnp.einsum("ij,ric->rjc", mixing_here, members, preferred_element_type=jnp.float32)
    totals = jnp.sum(members, axis=1, dtype=jnp.float32, keepdims=True)
    mixed = (combined + totals * keep_share[None]).astype(jnp.bfloat16)
    mixed = mixed.reshape(depth, mem, local, LANES).transpose(1, 0, 2, 3)
    mixed = exchange(mixed, "mem")

    gram = kernel(
        gram_kernel, vmem((BLOCK, LANES), jnp.float32), [VMEM] * 4,
        4 * depth * quantities * MEMBERS * LANES, state_bytes,
        [pltpu.VMEM((MEMBERS, quantities // halves * LANES), jnp.float32)] * 2,
    )(members, factor, pairs, total)
    gram = lax.psum(lax.psum(gram, "space_1"), "space_0")
    gram = kernel(
        spread_kernel, vmem((mem, BLOCK // 4, 4, LANES), jnp.float32), [VMEM],
        MEMBERS**2, 2 * mem * MEMBERS**2,
    )(gram)
    order = [i // 2 + (i + 1) % 2 * (mem // 2) for i in range(mem)]
    order = order[mem // 4 :] + order[: mem // 4]
    gram = exchange(gram, "mem", [order])
    prior_gram, posterior_gram = kernel(
        final_kernel, (square, square), [VMEM] * 3, 4 * MEMBERS**3, 16 * MEMBERS**2
    )(gram, mixing, turned)

    analysis = kernel(
        unpack_kernel, vmem((variables, local, cells), jnp.bfloat16), [VMEM],
        state_bytes, 2 * state_bytes,
    )(mixed)
    return (analysis.transpose(1, 0, 2), prior_gram, posterior_gram)


def solution(mesh):
    parts, mem, space = mesh.shape["parts"], mesh.shape["mem"], mesh.shape["space"]
    finer = Mesh(
        mesh.devices.reshape(parts, mem, space // 2, 2), ("parts", "mem", "space_0", "space_1")
    )

    def body(*args):
        return per_device(mem, *args)

    columns = ("parts", "space_0", "space_1")
    whole, rows, split = P("mem", None, columns), P("parts", None), P(None, columns)
    return jax.shard_map(
        body, mesh=finer, in_specs=(whole, rows, P(), split), out_specs=(whole, rows, rows),
        check_vma=False,
    )
```

```python
import functools

import jax
import jax.numpy as jnp
from jax import lax
from jax.experimental import pallas as pl
from jax.experimental.pallas import tpu as pltpu
from jax.sharding import Mesh
from jax.sharding import PartitionSpec as P


MEMBERS = 64
LANES = 128
GROUP = 4
BLOCK = 16
PACK_STEPS = 5
VMEM_LIMIT = 12 << 20
HIGHEST = lax.Precision.HIGHEST


SMEM = pl.BlockSpec(memory_space=pltpu.SMEM)
VMEM = pl.BlockSpec(memory_space=pltpu.VMEM)
HBM = pl.BlockSpec(memory_space=pltpu.HBM)


def exchange(array, axis, groups=None):
    return lax.all_to_all(
        array, axis, split_axis=0, concat_axis=0, tiled=True, axis_index_groups=groups
    )


def in_hbm(array):
    return pltpu.with_memory_space_constraint(array, pltpu.HBM)


def vmem(shape, dtype):
    return jax.ShapeDtypeStruct(shape, dtype)


def kernel(body, out_shape, in_specs, flops, moved, scratch=(), out_specs=None, **more):
    many = isinstance(out_shape, tuple)
    return pl.pallas_call(
        body, out_shape=out_shape, in_specs=in_specs, scratch_shapes=scratch,
        out_specs=out_specs or ((VMEM,) * len(out_shape) if many else VMEM),
        cost_estimate=pl.CostEstimate(flops=flops, bytes_accessed=moved, transcendentals=0),
        **{"compiler_params": pltpu.CompilerParams(vmem_limit_bytes=VMEM_LIMIT), **more},
    )


def rotate(array, by, axis):
    cut = array.shape[axis] - by
    parts = (array[cut:], array[:cut]) if axis == 0 else (array[:, cut:], array[:, :cut])
    return jnp.concatenate(parts, axis=axis)


def pack_kernel(x_ref, transform_ref, o_ref, keep_ref, mixing_ref, x, read_transform, sems, sem):
    depth, half = o_ref.shape[1], LANES // 2
    cuts = [depth * i // PACK_STEPS for i in range(PACK_STEPS + 1)]
    steps = [slice(a, b) for a, b in zip(cuts[:-1], cuts[1:], strict=True)]
    shifted = [slice(depth + s.start, depth + s.stop) for s in steps]
    reads = [
        [pltpu.make_async_copy(x_ref.at[s], x.at[s], sems.at[i, j]) for j, s in enumerate(both)]
        for i, both in enumerate(zip(steps, shifted, strict=True))
    ]
    mixing_read = pltpu.make_async_copy(transform_ref, read_transform, sem)
    for near_read, far_read in reads:
        near_read.start()
        far_read.start()
    mixing_read.start()
    mixing_read.wait()
    local, mem = o_ref.shape[2], o_ref.shape[0]
    mixing = rotate(rotate(read_transform[...].astype(jnp.float32), local, 0), local, 1)
    mixing_ref[...] = mixing.astype(mixing_ref.dtype)
    keep = (1.0 - jnp.sum(mixing.T, axis=1, keepdims=True)) / MEMBERS
    keep_ref[...] = jnp.broadcast_to(keep, keep_ref.shape)
    for (near_read, far_read), near, far in zip(reads, steps, shifted, strict=True):
        near_read.wait()
        far_read.wait()
        for tile in range(x.shape[2] // LANES):
            at = slice(tile * LANES, (tile + 1) * LANES)
            low, high = x[near, :, at], x[far, :, at]
            o_ref[2 * tile + 1, near] = jnp.concatenate([low[..., :half], high[..., :half]], axis=-1)
            o_ref[(2 * tile + 2) % mem, near] = jnp.concatenate([low[..., half:], high[..., half:]], axis=-1)


def unpack_kernel(x_ref, o_ref):
    depth, half = x_ref.shape[1], LANES // 2
    for tile in range(o_ref.shape[2] // LANES):
        at = slice(tile * LANES, (tile + 1) * LANES)
        left, right = x_ref[2 * tile + 1], x_ref[(2 * tile + 2) % x_ref.shape[0]]
        o_ref[:depth, :, at] = jnp.concatenate([left[..., :half], right[..., :half]], axis=-1)
        o_ref[depth:, :, at] = jnp.concatenate([left[..., half:], right[..., half:]], axis=-1)


def fold(gram, total):
    row = lax.broadcasted_iota(jnp.int32, (BLOCK, BLOCK), 0)
    column = lax.broadcasted_iota(jnp.int32, (BLOCK, BLOCK), 1)
    starts = range(0, MEMBERS, BLOCK)
    across = [gram[a : a + BLOCK, a + BLOCK :] for a in starts[:-1]]
    inner = [gram[a : a + BLOCK, a : a + BLOCK] for a in starts]
    pairs = [
        jnp.where(row < column, one, jnp.where(row > column, two, total))
        for one, two in zip(inner[::2], inner[1::2], strict=True)
    ]
    return jnp.concatenate([*across, *pairs], axis=1)


def unfold(packed):
    row = lax.broadcasted_iota(jnp.int32, (BLOCK, BLOCK), 0)
    column = lax.broadcasted_iota(jnp.int32, (BLOCK, BLOCK), 1)
    blocks = MEMBERS // BLOCK
    start, rows = 0, []
    pair_start = BLOCK * blocks * (blocks - 1) // 2
    for b in range(blocks):
        wide = MEMBERS - BLOCK * (b + 1)
        at = pair_start + BLOCK * (b // 2)
        pair = packed[:, at : at + BLOCK]
        pieces = [jnp.where(row < column if b % 2 == 0 else row > column, pair, 0.0)]
        if b:
            pieces.insert(0, jnp.zeros((BLOCK, BLOCK * b), jnp.float32))
        if wide:
            pieces.append(packed[:, start : start + wide])
        rows.append(jnp.concatenate(pieces, axis=1))
        start += wide
    half = jnp.concatenate(rows, axis=0)
    gram = half + half.T
    row = lax.broadcasted_iota(jnp.int32, gram.shape, 0)
    column = lax.broadcasted_iota(jnp.int32, gram.shape, 1)
    return jnp.where(row == column, -jnp.sum(gram, axis=1, keepdims=True), gram)


def prepare_kernel(
    mem_ref, operator_ref, weight_ref, transform_ref,
    factor_ref, pairs_ref, total_ref, mixing_ref, turned_ref,
):
    depth, quantities, _ = factor_ref.shape
    low = lax.broadcasted_iota(jnp.int32, (quantities, LANES), 1) < LANES // 2
    operator = operator_ref[...].astype(jnp.float32)
    for r in range(depth):
        factor_ref[r] = jnp.where(low, operator[:, r : r + 1], operator[:, depth + r : depth + r + 1])
    place = mem_ref[0, 0]
    tile = weight_ref[:, pl.ds(pl.multiple_of(place // 2 * LANES, LANES), LANES)]
    turned = pltpu.roll(tile, LANES // 2, 1)
    even = place % 2 == 0
    near, far = jnp.where(even, tile, turned), jnp.where(even, turned, tile)
    for pair in range(quantities // 2):
        one, two = near[2 * pair : 2 * pair + 1], far[2 * pair + 1 : 2 * pair + 2]
        pairs_ref[pair : pair + 1, :] = jnp.where(low[:1], one, two)
    total_ref[...] = jnp.full(total_ref.shape, jnp.sum(weight_ref[...]), jnp.float32)
    mixing = transform_ref[...].astype(jnp.float32)
    mixing_ref[...] = mixing
    turned_ref[...] = mixing.T


def gram_kernel(x_ref, factor_ref, weight_ref, total_ref, gram_ref, lhs, rhs):
    depth, quantities = factor_ref.shape[:2]
    low = lax.broadcasted_iota(jnp.int32, (MEMBERS, LANES), 1) < LANES // 2
    zero = jnp.zeros((MEMBERS, LANES), jnp.float32)
    for first in range(0, quantities, GROUP):

        def step(r, sums, first=first):
            x = x_ref[r].astype(jnp.float32)
            return tuple(
                s + x * factor_ref[r, pl.ds(first + i, 1), :] for i, s in enumerate(sums)
            )

        sums = lax.fori_loop(0, depth, step, (zero,) * GROUP, unroll=5)
        for i in range(0, GROUP, 2):
            one, two = sums[i], sums[i + 1]
            both = jnp.where(low, one, two) + pltpu.roll(jnp.where(low, two, one), LANES // 2, 1)
            departures = both - jnp.sum(both, axis=0, keepdims=True) / MEMBERS
            pair = (first + i) // 2
            at = slice(pair * LANES, (pair + 1) * LANES)
            rhs[:, at] = departures
            lhs[:, at] = departures * weight_ref[pair : pair + 1, :]
    gram = lax.dot_general(
        lhs[...], rhs[...], (((1,), (1,)), ((), ())), precision=HIGHEST,
        preferred_element_type=jnp.float32,
    )
    gram_ref[...] = fold(gram, total_ref[:1, :1])


def spread_kernel(gram_ref, o_ref):
    first = LANES - MEMBERS // 2
    scaled = gram_ref[...] / gram_ref[:1, first : first + 1]
    for i in range(BLOCK // 4):
        piece = scaled[4 * i : 4 * i + 4]
        o_ref[:, i] = jnp.broadcast_to(piece[None], (o_ref.shape[0], *piece.shape))


def final_kernel(local, gram_ref, mixing_ref, turned_ref, prior_ref, posterior_ref):
    pieces = [jnp.sum(gram_ref[:, i], axis=0) for i in range(gram_ref.shape[1])]
    gram = unfold(jnp.concatenate(pieces, axis=0))
    back = MEMBERS - local
    prior_ref[...] = rotate(rotate(gram, back, 0), back, 1)
    dot = functools.partial(jnp.dot, precision=HIGHEST, preferred_element_type=jnp.float32)
    posterior = dot(dot(turned_ref[...], gram), mixing_ref[...])
    posterior_ref[...] = rotate(rotate(posterior, back, 0), back, 1)


def per_device(mem, ensemble, transform, obs_operator, obs_weight):
    local, variables, cells = ensemble.shape
    quantities = obs_operator.shape[0]
    halves = LANES * mem // cells
    depth = variables // halves
    place = lax.axis_index("mem").astype(jnp.int32).reshape(1, 1)
    state_bytes = 2 * ensemble.size
    square = vmem((MEMBERS, MEMBERS), jnp.float32)

    shapes = (
        vmem((mem, depth, local, LANES), jnp.bfloat16), vmem((MEMBERS, LANES), jnp.float32),
        vmem(transform.shape, transform.dtype),
    )
    blocks, keep_share, mixing_here = kernel(
        pack_kernel, shapes, [HBM, HBM], state_bytes, 2 * state_bytes,
        [
            pltpu.VMEM((variables, local, cells), jnp.bfloat16),
            pltpu.VMEM(transform.shape, transform.dtype),
            pltpu.SemaphoreType.DMA((PACK_STEPS, 2)), pltpu.SemaphoreType.DMA,
        ],
    )(in_hbm(ensemble.transpose(1, 0, 2)), in_hbm(transform))
    last_first = [(i - 1) % mem for i in range(mem)]
    members = exchange(blocks, "mem", [last_first])

    shapes = ((depth, quantities, LANES), (quantities // halves, LANES), (8, LANES))
    factor, pairs, total, mixing, turned = kernel(
        prepare_kernel, (*(vmem(s, jnp.float32) for s in shapes), square, square),
        [SMEM, VMEM, VMEM, VMEM], 4 * obs_weight.size, 8 * obs_weight.size,
    )(place, obs_operator, obs_weight, mixing_here)

    members = members.transpose(1, 0, 2, 3).reshape(depth, MEMBERS, LANES)
    combined = jnp.einsum("ij,ric->rjc", mixing_here, members, preferred_element_type=jnp.float32)
    totals = jnp.sum(members, axis=1, dtype=jnp.float32, keepdims=True)
    mixed = (combined + totals * keep_share[None]).astype(jnp.bfloat16)
    mixed = mixed.reshape(depth, mem, local, LANES).transpose(1, 0, 2, 3)
    mixed = exchange(mixed, "mem", [last_first])

    gram = kernel(
        gram_kernel, vmem((BLOCK, LANES), jnp.float32), [VMEM] * 4,
        4 * depth * quantities * MEMBERS * LANES, state_bytes,
        [pltpu.VMEM((MEMBERS, quantities // halves * LANES), jnp.float32)] * 2,
    )(members, factor, pairs, total)
    gram = lax.psum(lax.psum(gram, "space_1"), "space_0")
    gram = kernel(
        spread_kernel, vmem((mem, BLOCK // 4, 4, LANES), jnp.float32), [VMEM],
        MEMBERS**2, 2 * mem * MEMBERS**2,
    )(gram)
    far_first = [i // 2 + (i + 1) % 2 * (mem // 2) for i in range(mem)]
    gram = exchange(gram, "mem", [far_first])
    prior_gram, posterior_gram = kernel(
        functools.partial(final_kernel, local), (square, square), [VMEM] * 3, 4 * MEMBERS**3, 16 * MEMBERS**2
    )(gram, mixing, turned)

    analysis = kernel(
        unpack_kernel, vmem((variables, local, cells), jnp.bfloat16), [VMEM],
        state_bytes, 2 * state_bytes,
    )(mixed)
    return (analysis.transpose(1, 0, 2), prior_gram, posterior_gram)


def solution(mesh):
    parts, mem, space = mesh.shape["parts"], mesh.shape["mem"], mesh.shape["space"]
    finer = Mesh(
        mesh.devices.reshape(parts, mem, space // 2, 2), ("parts", "mem", "space_0", "space_1")
    )

    def body(*args):
        return per_device(mem, *args)

    columns = ("parts", "space_0", "space_1")
    whole, rows, split = P("mem", None, columns), P("parts", None), P(None, columns)
    return jax.shard_map(
        body, mesh=finer, in_specs=(whole, rows, P(), split), out_specs=(whole, rows, rows),
        check_vma=False,
    )
```

```python
import functools

import jax
import jax.numpy as jnp
from jax import lax
from jax.experimental import pallas as pl
from jax.experimental.pallas import tpu as pltpu
from jax.sharding import Mesh
from jax.sharding import PartitionSpec as P


MEMBERS = 64
LANES = 128
GROUP = 4
BLOCK = 16
PACK_STEPS = 2
VMEM_LIMIT = 12 << 20
HIGHEST = lax.Precision.HIGHEST


SMEM = pl.BlockSpec(memory_space=pltpu.SMEM)
VMEM = pl.BlockSpec(memory_space=pltpu.VMEM)
HBM = pl.BlockSpec(memory_space=pltpu.HBM)


def exchange(array, axis, groups=None):
    return lax.all_to_all(
        array, axis, split_axis=0, concat_axis=0, tiled=True, axis_index_groups=groups
    )


def in_hbm(array):
    return pltpu.with_memory_space_constraint(array, pltpu.HBM)


def vmem(shape, dtype):
    return jax.ShapeDtypeStruct(shape, dtype)


def kernel(body, out_shape, in_specs, flops, moved, scratch=(), out_specs=None, **more):
    many = isinstance(out_shape, tuple)
    return pl.pallas_call(
        body, out_shape=out_shape, in_specs=in_specs, scratch_shapes=scratch,
        out_specs=out_specs or ((VMEM,) * len(out_shape) if many else VMEM),
        cost_estimate=pl.CostEstimate(flops=flops, bytes_accessed=moved, transcendentals=0),
        **{"compiler_params": pltpu.CompilerParams(vmem_limit_bytes=VMEM_LIMIT), **more},
    )


def rotate(array, by, axis):
    cut = array.shape[axis] - by
    parts = (array[cut:], array[:cut]) if axis == 0 else (array[:, cut:], array[:, :cut])
    return jnp.concatenate(parts, axis=axis)


def pack_kernel(x_ref, transform_ref, o_ref, keep_ref, mixing_ref, x, read_transform, sems, sem):
    depth, half = o_ref.shape[1], LANES // 2
    cuts = [depth * i // PACK_STEPS for i in range(PACK_STEPS + 1)]
    steps = [slice(a, b) for a, b in zip(cuts[:-1], cuts[1:], strict=True)]
    shifted = [slice(depth + s.start, depth + s.stop) for s in steps]
    reads = [
        [pltpu.make_async_copy(x_ref.at[s], x.at[s], sems.at[i, j]) for j, s in enumerate(both)]
        for i, both in enumerate(zip(steps, shifted, strict=True))
    ]
    mixing_read = pltpu.make_async_copy(transform_ref, read_transform, sem)
    mixing_read.start()
    for near_read, far_read in reads:
        near_read.start()
        far_read.start()
    mixing_read.wait()
    local, mem = o_ref.shape[2], o_ref.shape[0]
    mixing = rotate(rotate(read_transform[...].astype(jnp.float32), local, 0), local, 1)
    mixing_ref[...] = mixing.astype(mixing_ref.dtype)
    keep = (1.0 - jnp.sum(mixing.T, axis=1, keepdims=True)) / MEMBERS
    keep_ref[...] = jnp.broadcast_to(keep, keep_ref.shape)
    for (near_read, far_read), near, far in zip(reads, steps, shifted, strict=True):
        near_read.wait()
        far_read.wait()
        for tile in range(x.shape[2] // LANES):
            at = slice(tile * LANES, (tile + 1) * LANES)
            low, high = x[near, :, at], x[far, :, at]
            o_ref[2 * tile + 1, near] = jnp.concatenate([low[..., :half], high[..., :half]], axis=-1)
            o_ref[(2 * tile + 2) % mem, near] = jnp.concatenate([low[..., half:], high[..., half:]], axis=-1)


def unpack_kernel(x_ref, o_ref):
    depth, half = x_ref.shape[1], LANES // 2
    for tile in range(o_ref.shape[2] // LANES):
        at = slice(tile * LANES, (tile + 1) * LANES)
        left, right = x_ref[2 * tile + 1], x_ref[(2 * tile + 2) % x_ref.shape[0]]
        o_ref[:depth, :, at] = jnp.concatenate([left[..., :half], right[..., :half]], axis=-1)
        o_ref[depth:, :, at] = jnp.concatenate([left[..., half:], right[..., half:]], axis=-1)


def fold(gram, total):
    row = lax.broadcasted_iota(jnp.int32, (BLOCK, BLOCK), 0)
    column = lax.broadcasted_iota(jnp.int32, (BLOCK, BLOCK), 1)
    starts = range(0, MEMBERS, BLOCK)
    across = [gram[a : a + BLOCK, a + BLOCK :] for a in starts[:-1]]
    inner = [gram[a : a + BLOCK, a : a + BLOCK] for a in starts]
    pairs = [
        jnp.where(row < column, one, jnp.where(row > column, two, total))
        for one, two in zip(inner[::2], inner[1::2], strict=True)
    ]
    return jnp.concatenate([*across, *pairs], axis=1)


def unfold(packed):
    row = lax.broadcasted_iota(jnp.int32, (BLOCK, BLOCK), 0)
    column = lax.broadcasted_iota(jnp.int32, (BLOCK, BLOCK), 1)
    blocks = MEMBERS // BLOCK
    start, rows = 0, []
    pair_start = BLOCK * blocks * (blocks - 1) // 2
    for b in range(blocks):
        wide = MEMBERS - BLOCK * (b + 1)
        at = pair_start + BLOCK * (b // 2)
        pair = packed[:, at : at + BLOCK]
        pieces = [jnp.where(row < column if b % 2 == 0 else row > column, pair, 0.0)]
        if b:
            pieces.insert(0, jnp.zeros((BLOCK, BLOCK * b), jnp.float32))
        if wide:
            pieces.append(packed[:, start : start + wide])
        rows.append(jnp.concatenate(pieces, axis=1))
        start += wide
    half = jnp.concatenate(rows, axis=0)
    gram = half + half.T
    row = lax.broadcasted_iota(jnp.int32, gram.shape, 0)
    column = lax.broadcasted_iota(jnp.int32, gram.shape, 1)
    return jnp.where(row == column, -jnp.sum(gram, axis=1, keepdims=True), gram)


def prepare_kernel(
    mem_ref, operator_ref, weight_ref, transform_ref,
    factor_ref, pairs_ref, total_ref, mixing_ref, turned_ref,
):
    depth, quantities, _ = factor_ref.shape
    low = lax.broadcasted_iota(jnp.int32, (quantities, LANES), 1) < LANES // 2
    operator = operator_ref[...].astype(jnp.float32)
    for r in range(depth):
        factor_ref[r] = jnp.where(low, operator[:, r : r + 1], operator[:, depth + r : depth + r + 1])
    place = mem_ref[0, 0]
    tile = weight_ref[:, pl.ds(pl.multiple_of(place // 2 * LANES, LANES), LANES)]
    turned = pltpu.roll(tile, LANES // 2, 1)
    even = place % 2 == 0
    near, far = jnp.where(even, tile, turned), jnp.where(even, turned, tile)
    for pair in range(quantities // 2):
        one, two = near[2 * pair : 2 * pair + 1], far[2 * pair + 1 : 2 * pair + 2]
        pairs_ref[pair : pair + 1, :] = jnp.where(low[:1], one, two)
    total_ref[...] = jnp.full(total_ref.shape, jnp.sum(weight_ref[...]), jnp.float32)
    mixing = transform_ref[...].astype(jnp.float32)
    mixing_ref[...] = mixing
    turned_ref[...] = mixing.T


def gram_kernel(x_ref, factor_ref, weight_ref, total_ref, gram_ref, lhs, rhs):
    depth, quantities = factor_ref.shape[:2]
    low = lax.broadcasted_iota(jnp.int32, (MEMBERS, LANES), 1) < LANES // 2
    zero = jnp.zeros((MEMBERS, LANES), jnp.float32)
    for first in range(0, quantities, GROUP):

        def step(r, sums, first=first):
            x = x_ref[r].astype(jnp.float32)
            return tuple(
                s + x * factor_ref[r, pl.ds(first + i, 1), :] for i, s in enumerate(sums)
            )

        sums = lax.fori_loop(0, depth, step, (zero,) * GROUP, unroll=5)
        for i in range(0, GROUP, 2):
            one, two = sums[i], sums[i + 1]
            both = jnp.where(low, one, two) + pltpu.roll(jnp.where(low, two, one), LANES // 2, 1)
            departures = both - jnp.sum(both, axis=0, keepdims=True) / MEMBERS
            pair = (first + i) // 2
            at = slice(pair * LANES, (pair + 1) * LANES)
            rhs[:, at] = departures
            lhs[:, at] = departures * weight_ref[pair : pair + 1, :]
    gram = lax.dot_general(
        lhs[...], rhs[...], (((1,), (1,)), ((), ())), precision=HIGHEST,
        preferred_element_type=jnp.float32,
    )
    gram_ref[...] = fold(gram, total_ref[:1, :1])


def spread_kernel(gram_ref, o_ref):
    first = LANES - MEMBERS // 2
    scaled = gram_ref[...] / gram_ref[:1, first : first + 1]
    for i in range(BLOCK // 4):
        piece = scaled[4 * i : 4 * i + 4]
        o_ref[:, i] = jnp.broadcast_to(piece[None], (o_ref.shape[0], *piece.shape))


def final_kernel(local, gram_ref, mixing_ref, turned_ref, prior_ref, posterior_ref):
    pieces = [jnp.sum(gram_ref[:, i], axis=0) for i in range(gram_ref.shape[1])]
    gram = unfold(jnp.concatenate(pieces, axis=0))
    back = MEMBERS - local
    prior_ref[...] = rotate(rotate(gram, back, 0), back, 1)
    dot = functools.partial(jnp.dot, precision=HIGHEST, preferred_element_type=jnp.float32)
    posterior = dot(dot(turned_ref[...], gram), mixing_ref[...])
    posterior_ref[...] = rotate(rotate(posterior, back, 0), back, 1)


def per_device(mem, ensemble, transform, obs_operator, obs_weight):
    local, variables, cells = ensemble.shape
    quantities = obs_operator.shape[0]
    halves = LANES * mem // cells
    depth = variables // halves
    place = lax.axis_index("mem").astype(jnp.int32).reshape(1, 1)
    state_bytes = 2 * ensemble.size
    square = vmem((MEMBERS, MEMBERS), jnp.float32)

    shapes = (
        vmem((mem, depth, local, LANES), jnp.bfloat16), vmem((MEMBERS, LANES), jnp.float32),
        vmem(transform.shape, transform.dtype),
    )
    blocks, keep_share, mixing_here = kernel(
        pack_kernel, shapes, [HBM, HBM], state_bytes, 2 * state_bytes,
        [
            pltpu.VMEM((variables, local, cells), jnp.bfloat16),
            pltpu.VMEM(transform.shape, transform.dtype),
            pltpu.SemaphoreType.DMA((PACK_STEPS, 2)), pltpu.SemaphoreType.DMA,
        ],
    )(in_hbm(ensemble.transpose(1, 0, 2)), in_hbm(transform))
    last_first = [(i - 1) % mem for i in range(mem)]
    members = exchange(blocks, "mem", [last_first])

    shapes = ((depth, quantities, LANES), (quantities // halves, LANES), (8, LANES))
    factor, pairs, total, mixing, turned = kernel(
        prepare_kernel, (*(vmem(s, jnp.float32) for s in shapes), square, square),
        [SMEM, VMEM, VMEM, VMEM], 4 * obs_weight.size, 8 * obs_weight.size,
    )(place, obs_operator, obs_weight, mixing_here)

    members = members.transpose(1, 0, 2, 3).reshape(depth, MEMBERS, LANES)
    combined = jnp.einsum("ij,ric->rjc", mixing_here, members, preferred_element_type=jnp.float32)
    totals = jnp.sum(members, axis=1, dtype=jnp.float32, keepdims=True)
    mixed = (combined + totals * keep_share[None]).astype(jnp.bfloat16)
    mixed = mixed.reshape(depth, mem, local, LANES).transpose(1, 0, 2, 3)
    mixed = exchange(mixed, "mem", [last_first])

    gram = kernel(
        gram_kernel, vmem((BLOCK, LANES), jnp.float32), [VMEM] * 4,
        4 * depth * quantities * MEMBERS * LANES, state_bytes,
        [pltpu.VMEM((MEMBERS, quantities // halves * LANES), jnp.float32)] * 2,
    )(members, factor, pairs, total)
    gram = lax.psum(lax.psum(gram, "space_1"), "space_0")
    gram = kernel(
        spread_kernel, vmem((mem, BLOCK // 4, 4, LANES), jnp.float32), [VMEM],
        MEMBERS**2, 2 * mem * MEMBERS**2,
    )(gram)
    order = [i // 2 + (i + 1) % 2 * (mem // 2) for i in range(mem)]
    gram = exchange(gram, "mem", [order[2:] + order[:2]])
    prior_gram, posterior_gram = kernel(
        functools.partial(final_kernel, local), (square, square), [VMEM] * 3, 4 * MEMBERS**3, 16 * MEMBERS**2
    )(gram, mixing, turned)

    analysis = kernel(
        unpack_kernel, vmem((variables, local, cells), jnp.bfloat16), [VMEM],
        state_bytes, 2 * state_bytes,
    )(mixed)
    return (analysis.transpose(1, 0, 2), prior_gram, posterior_gram)


def solution(mesh):
    parts, mem, space = mesh.shape["parts"], mesh.shape["mem"], mesh.shape["space"]
    finer = Mesh(
        mesh.devices.reshape(parts, mem, space // 2, 2), ("parts", "mem", "space_0", "space_1")
    )

    def body(*args):
        return per_device(mem, *args)

    columns = ("parts", "space_0", "space_1")
    whole, rows, split = P("mem", None, columns), P("parts", None), P(None, columns)
    return jax.shard_map(
        body, mesh=finer, in_specs=(whole, rows, P(), split), out_specs=(whole, rows, rows),
        check_vma=False,
    )
```
